128 devices in a mesh: env: 8 (over z, core), tm: 16 (over y, x).
Axes of the slice: x: 4, y: 4, z: 4, core: 2. Of those that a mesh axis runs over, the one named last changes fastest.
Arguments:
- observations: bfloat16 [16, 12288, 2048], P('env', 'tm'), may hold values from -6 to 6
- stored_values: float32 [16, 12288], P('env', 'tm'), may hold values from -3.6 to 3.6
- rewards: float32 [16, 12288], P('env', 'tm'), may hold values from -0.18 to 0.18
- episode_ends: int32 [16, 12288], P('env', 'tm'), may hold values 0 or 1
- stale_list: int32 [8, 16, 12], P('env', 'tm'), may hold values from -1 to 11, as said below
- discount_horizon: float32 [16], P('env'), may hold values from 10 to 98304
- trace_horizon: float32 [16], P('env'), may hold values from 10 to 98304
- bootstrap: float32 [16], P('env'), may hold values from -3.6 to 3.6
- norm_gain: float32 [2048], replicated, may hold values from 0.1 to 1.9
- input_weight: bfloat16 [2048, 4096], replicated, may hold values from -0.125 to 0.125
- value_head: bfloat16 [4096], replicated, may hold values from -0.09375 to 0.09375
Outputs:
- targets: float32 [16, 12288], P('env', 'tm')
- advantages: float32 [16, 12288], P('env', 'tm')
The draws below stay inside these ranges and needn't reach their ends.
Inputs may be any that keep to these rules, and one draw needn't show every extreme that they name: `stale_list`: for each device (first two indices: env shard, time shard) the last dimension lists distinct local block numbers e * 6 + k (e an environment row within the env shard, k a block of 128 steps within the time shard), followed by -1 entries; on some device all 12 blocks are listed.
All inputs are finite; a program needn't handle non-finite values. No bound on the sum of `episode_ends` on one device may be relied on, other than what follows from the above.
Results may differ from the reference program's by a relative error of at most 0.0018.
Values may be sent and summed in bfloat16 or wider, within the bound.
A program may use at most 128 MiB of HBM per device.

```python
import jax
import jax.numpy as jnp
from jax import lax

D = 2048
FF = 4096
BLOCK = 128
ENV_DEV = 2
NB = 6
BLK_DEV = 12
SEQ = 12288
B = 16
N_ENV = 8
N_TM = 16


def draw_stale_list(key, part):
    device_count = N_ENV * N_TM
    device_keys = jax.random.split(jax.random.fold_in(key, 11), device_count)
    shuffled = jax.vmap(lambda one_key: jax.random.permutation(one_key, BLK_DEV))(device_keys)
    first_count = jax.random.randint(jax.random.fold_in(key, 12), (device_count,), 0, BLK_DEV + 1)
    second_count = jax.random.randint(jax.random.fold_in(key, 13), (device_count,), 0, BLK_DEV + 1)
    counts = jnp.minimum(first_count, second_count)
    busiest = jax.random.randint(jax.random.fold_in(key, 14), (), 0, device_count)
    counts = jnp.where(jnp.arange(device_count) == busiest, BLK_DEV, counts)
    listed = jnp.where(jnp.arange(BLK_DEV)[None, :] < counts[:, None], shuffled, -1)
    return listed.reshape(N_ENV, N_TM, BLK_DEV).astype(jnp.int32)


def draw_rewards(key, part):
    env_position = jnp.arange(B, dtype=jnp.float32) / max(B - 1, 1)
    scales = 0.005 * 9.0 ** env_position
    draw_noise = jnp.clip(jax.random.normal(jax.random.fold_in(key, 32), (B, SEQ), jnp.float32), -4.0, 4.0)
    return (draw_noise * scales[:, None]).astype(jnp.float32)


def horizon_draw(key, salt):
    slow_share = 0.5
    is_slow = jax.random.bernoulli(jax.random.fold_in(key, 21), slow_share, (B,))
    level = jax.random.uniform(jax.random.fold_in(key, salt), (B,), jnp.float32, 0.0, 1.0)
    fast_value = 10.0 * 4.0 ** level
    slow_value = 2.0 * SEQ * 4.0 ** level
    return jnp.where(is_slow, slow_value, fast_value).astype(jnp.float32)


def draw_discount_horizon(key, part):
    return horizon_draw(key, 22)


def draw_trace_horizon(key, part):
    return horizon_draw(key, 23)


def set_ends(values, own_key, low, largest):
    longest = values.shape.index(max(values.shape))
    spots = []
    for shift in (0, 1):
        where = [jax.random.randint(jax.random.fold_in(own_key, axis), (), 0, length) for axis, length in enumerate(values.shape)]
        where[longest] = (where[longest] + shift) % values.shape[longest]
        spots.append(tuple(where))
    return values.at[spots[0]].set(low).at[spots[1]].set(largest)


def levels(rng, shape, pieces, least, high):
    factor_of = 1.0
    for dim, parts in pieces:
        heights = jax.random.uniform(jax.random.fold_in(jax.random.fold_in(rng, 6), dim), (parts,), jnp.float32, least / len(pieces), high / len(pieces))
        factor_of = factor_of * jnp.repeat(jnp.exp(heights), shape[dim] // parts).reshape((-1,) + (1,) * (len(shape) - 1 - dim))
    return factor_of


def scatter_about(rng, extent, deviation, most, cuts=(), kind=jnp.bfloat16):
    loudness = levels(rng, extent, cuts, -0.22, 0.18) if cuts else 1.0
    values = jax.random.normal(rng, extent, jnp.float32) * deviation * loudness
    return jnp.minimum(jnp.maximum(values, -most), most).astype(kind)


def setup_inputs(seed: int = 0) -> dict:
    streams_of = jax.random.split(jax.random.key(seed), 12)
    observations = scatter_about(streams_of[0], (B, SEQ, D), 1.0, 6.0, ((0, 8), (1, 16)))
    stored_values = scatter_about(streams_of[1], (B, SEQ), 0.6, 3.6, ((0, 8), (1, 16)), jnp.float32)
    rewards = draw_rewards(jax.random.fold_in(streams_of[11], 71), 0)
    episode_ends = set_ends((jax.random.randint(streams_of[3], (B, SEQ), 0, SEQ // 2) < 1).astype(jnp.int32), jax.random.fold_in(streams_of[3], 1), 0, 1)
    stale_list = draw_stale_list(jax.random.fold_in(streams_of[11], 71), 0)
    discount_horizon = draw_discount_horizon(jax.random.fold_in(streams_of[11], 71), 0)
    trace_horizon = draw_trace_horizon(jax.random.fold_in(streams_of[11], 71), 0)
    bootstrap = scatter_about(streams_of[7], (B,), 0.6, 3.6, ((0, 8),), jnp.float32)
    norm_gain = jnp.clip(1.0 + 0.18 * jax.random.normal(streams_of[8], (D,), jnp.float32), 0.1, 1.9)
    input_weight = scatter_about(streams_of[9], (D, FF), D ** -0.5, 0.125)
    value_head = scatter_about(streams_of[10], (FF,), FF ** -0.5, 0.09375)
    return {"observations": observations, "stored_values": stored_values, "rewards": rewards, "episode_ends": episode_ends, "stale_list": stale_list, "discount_horizon": discount_horizon, "trace_horizon": trace_horizon, "bootstrap": bootstrap, "norm_gain": norm_gain, "input_weight": input_weight, "value_head": value_head}


def critic_rows(block_rows, norm_gain, input_weight, value_head):
    widened = block_rows.astype(jnp.float32)
    square_mean = lax.optimization_barrier(jnp.mean(widened * widened, axis=-1, keepdims=True))
    normed = (widened * lax.rsqrt(square_mean + 1e-05) * norm_gain).astype(jnp.bfloat16)
    hidden = jnp.dot(normed, input_weight, preferred_element_type=jnp.float32)
    active = jax.nn.silu(hidden).astype(jnp.bfloat16)
    return jnp.dot(active, value_head, preferred_element_type=jnp.float32)

def reference(observations, stored_values, rewards, episode_ends, stale_list, discount_horizon, trace_horizon, bootstrap, norm_gain, input_weight, value_head):
    env_total = ENV_DEV * N_ENV
    block_ids = jnp.arange(ENV_DEV * NB, dtype=jnp.int32)
    listed = jnp.any(stale_list[..., :, None] == block_ids[None, None, None, :], axis=-2)
    stale_blocks = listed.reshape(N_ENV, N_TM, ENV_DEV, NB).transpose(0, 2, 1, 3).reshape(env_total, N_TM * NB)
    grouped = observations.reshape(env_total * N_TM * NB, BLOCK, D)
    stale_flags = stale_blocks.reshape(-1)

    def refresh(element):
        block_rows, is_stale = element
        return lax.cond(is_stale, lambda rows_in: critic_rows(rows_in, norm_gain, input_weight, value_head), lambda rows_in: jnp.zeros((BLOCK,), jnp.float32), block_rows)
    fresh = lax.map(refresh, (grouped, stale_flags)).reshape(env_total, SEQ)
    stale_mask = jnp.repeat(stale_blocks, BLOCK, axis=1)
    values = jnp.where(stale_mask, fresh, stored_values)
    next_values = jnp.concatenate([values[:, 1:], bootstrap[:, None]], axis=1)
    discount = 1.0 - 1.0 / discount_horizon
    trace_rate = 1.0 - 1.0 / trace_horizon
    continuing = 1.0 - episode_ends.astype(jnp.float32)
    td_error = rewards + discount[:, None] * continuing * next_values - values
    decay_rate = discount[:, None] * trace_rate[:, None] * continuing

    def backward(running, element):
        error_now, decay_now = element
        updated = error_now + decay_now * running
        return (updated, updated)
    start = jnp.zeros((env_total,), jnp.float32)
    unused, adv_steps = lax.scan(backward, start, (td_error.T, decay_rate.T), reverse=True)
    adv = adv_steps.T
    targets = adv + values
    adv_mean = jnp.mean(adv)
    centered = adv - adv_mean
    adv_var = jnp.mean(centered * centered)
    advantages = centered / jnp.sqrt(adv_var + 1e-05)
    return (targets, advantages)
```

```python
import functools

import jax
import jax.numpy as jnp
from jax import lax
from jax.experimental import pallas as pl
from jax.experimental.pallas import tpu as pltpu
from jax.sharding import PartitionSpec as P

BLOCK = 128
CHUNK = 512
PIECE = 32
FIELDS = 16
MESH = pl.DeviceIdType.MESH


def spread(pair, rows, half):
    row = lax.broadcasted_iota(jnp.int32, (rows, BLOCK), 0)
    return jnp.where(row < half, pair[0], pair[1])


def shifted_left(value, by):
    return pltpu.roll(value, value.shape[1] - by, 1)


def shifted_up(value, by):
    return pltpu.roll(value, value.shape[0] - by, 0)


def sweep_kernel(
    listed,
    discount_horizon,
    trace_horizon,
    bootstrap,
    obs,
    weight,
    stored,
    rewards,
    ends,
    gain,
    head,
    offset_ref,
    factor_ref,
    value_ref,
    message_ref,
    raw,
    held,
    normed_a,
    normed_b,
    fresh,
    packed,
    raw_sem,
    held_sem,
):
    slots, _, features = raw.shape
    width = held.shape[1]
    chunks = width // CHUNK
    env_rows, steps = stored.shape
    per_row = steps // BLOCK
    count = jnp.int32(0)
    for j in range(slots):
        count += (listed[0, 0, j] >= 0).astype(jnp.int32)
    groups = (count + 1) // 2

    def raw_copy(slot):
        block = jnp.maximum(listed[0, 0, slot], 0)
        return pltpu.make_async_copy(obs.at[block], raw.at[slot], raw_sem.at[slot])

    def held_copy(c):
        part = pl.ds(c * CHUNK, CHUNK)
        return pltpu.make_async_copy(
            weight.at[:, part], held.at[:, part], held_sem.at[c]
        )

    def start_raw(slot):
        @pl.when(slot < count)
        def _():
            raw_copy(slot).start()

    def wait_group(group):
        for side in range(2):
            slot = 2 * group + side

            @pl.when(slot < count)
            def _():
                raw_copy(slot).wait()

    def normalize(group, piece, target):
        per_block = BLOCK // PIECE
        slot = jnp.minimum(2 * group + piece // per_block, slots - 1)
        rows = pl.ds((piece % per_block) * PIECE, PIECE)
        widened = raw[slot, rows, :].astype(jnp.float32)
        square_mean = jnp.mean(widened * widened, axis=-1, keepdims=True)
        scaled = widened * lax.rsqrt(square_mean + 1e-05) * gain[...]
        target[pl.ds(piece * PIECE, PIECE), :] = scaled.astype(jnp.bfloat16)

    def run_group(group, source, target, may_be_first):
        pieces = 2 * BLOCK // PIECE
        total = jnp.zeros((2 * BLOCK, BLOCK), jnp.float32)
        for c in range(chunks):
            if may_be_first:

                @pl.when(group == 0)
                def _():
                    held_copy(c).wait()

            part = pl.ds(c * CHUNK, CHUNK)
            hidden = jnp.dot(
                source[...], held[:, part], preferred_element_type=jnp.float32
            )
            active = (0.5 * hidden) * (1.0 + jnp.tanh(0.5 * hidden))
            active = active.astype(jnp.bfloat16).astype(jnp.float32) * head[:, part]
            for k in range(CHUNK // BLOCK):
                total += active[:, k * BLOCK : (k + 1) * BLOCK]
            for piece in range(c * pieces // chunks, (c + 1) * pieces // chunks):
                normalize(group + 1, piece, target)
        for side in range(2):
            slot = 2 * group + side
            scores = jnp.sum(
                total[side * BLOCK : (side + 1) * BLOCK].T, axis=0, keepdims=True
            )

            @pl.when(slot < count)
            def _():
                fresh[pl.ds(listed[0, 0, jnp.minimum(slot, slots - 1)], 1), :] = scores

    for e in range(env_rows):
        for k in range(per_row):
            row, part = pl.ds(e * per_row + k, 1), pl.ds(k * BLOCK, BLOCK)
            fresh[row, :] = stored[e : e + 1, part]
            packed[0, row, :] = rewards[e : e + 1, part]
            packed[1, row, :] = 1.0 - ends[e : e + 1, part].astype(jnp.float32)

    @pl.when(count > 0)
    def _():
        for slot in range(2):
            start_raw(slot)
        for c in range(chunks):
            held_copy(c).start()
            if c == chunks // 2:
                for slot in range(2, 4):
                    start_raw(slot)
        for slot in range(4, slots):
            start_raw(slot)
        wait_group(0)
        for piece in range(2 * BLOCK // PIECE):
            normalize(0, piece, normed_a)

        def two_groups(i, carry):
            wait_group(2 * i + 1)
            run_group(2 * i, normed_a, normed_b, True)

            @pl.when(2 * i + 1 < groups)
            def _():
                wait_group(2 * i + 2)
                run_group(2 * i + 1, normed_b, normed_a, False)

            return carry

        lax.fori_loop(0, (groups + 1) // 2, two_groups, 0)

    rows = fresh.shape[0]
    half = per_row
    value = fresh[...]
    lane = lax.broadcasted_iota(jnp.int32, (rows, BLOCK), 1)
    row = lax.broadcasted_iota(jnp.int32, (rows, BLOCK), 0)
    place = jnp.where(row < half, row, row - half)
    discount = 1.0 - 1.0 / spread((discount_horizon[0], discount_horizon[1]), rows, half)
    trace = 1.0 - 1.0 / spread((trace_horizon[0], trace_horizon[1]), rows, half)
    live = row < env_rows * half
    reward = jnp.where(live, packed[0], 0.0)
    going = jnp.where(live, packed[1], 0.0)
    value = jnp.where(live, value, 0.0)
    turned = shifted_left(value, 1)
    following = jnp.where(lane < BLOCK - 1, turned, shifted_up(turned, 1))
    last = (lane == BLOCK - 1) & (place == half - 1)
    following = jnp.where(last, value, following)
    factor = discount * trace * going
    offset = reward + discount * going * following - value
    by = 1
    while by < BLOCK:
        inside = lane < BLOCK - by
        offset = offset + factor * jnp.where(inside, shifted_left(offset, by), 0.0)
        factor = factor * jnp.where(inside, shifted_left(factor, by), 1.0)
        by *= 2
    row_factor = jnp.broadcast_to(factor[:, :1], (rows, BLOCK))
    row_offset = jnp.broadcast_to(offset[:, :1], (rows, BLOCK))
    by = 1
    while by < half:
        inside = place + by < half
        row_offset = row_offset + row_factor * jnp.where(
            inside, shifted_up(row_offset, by), 0.0
        )
        row_factor = row_factor * jnp.where(inside, shifted_up(row_factor, by), 1.0)
        by *= 2
    inside = place + 1 < half
    offset = offset + factor * jnp.where(inside, shifted_up(row_offset, 1), 0.0)
    factor = factor * jnp.where(inside, shifted_up(row_factor, 1), 1.0)

    packed[0] = offset
    packed[1] = factor
    fresh[...] = value
    lanes = lax.broadcasted_iota(jnp.int32, (1, BLOCK), 1)
    line = jnp.zeros((1, BLOCK), jnp.float32)
    for e in range(env_rows):
        mine = live & (row >= e * half) & (row < (e + 1) * half)

        def mean_of(array):
            return jnp.sum(jnp.where(mine, array, 0.0), keepdims=True) / steps

        mean_offset, mean_factor = mean_of(offset), mean_of(factor)
        near, far = offset - mean_offset, factor - mean_factor
        items = (
            row_offset[e * half : e * half + 1, :1],
            row_factor[e * half : e * half + 1, :1],
            value[e * half : e * half + 1, :1],
            value[(e + 1) * half - 1 : (e + 1) * half, BLOCK - 1 :],
            mean_offset,
            mean_factor,
            mean_of(near * near),
            mean_of(near * far),
            mean_of(far * far),
            1.0 / trace[e * half : e * half + 1, :1],
            jnp.full((1, 1), bootstrap[e], jnp.float32),
        )
        for k, item in enumerate(items):
            line = jnp.where(lanes == e * FIELDS + k, item, line)
        for k in range(per_row):
            source, part = pl.ds(e * per_row + k, 1), pl.ds(k * BLOCK, BLOCK)
            offset_ref[e : e + 1, part] = packed[0, source, :]
            factor_ref[e : e + 1, part] = packed[1, source, :]
            value_ref[e : e + 1, part] = fresh[source, :]
    message_ref[...] = line.reshape(message_ref.shape)


def peers(index):
    z, y, x, core = index // 32, index // 8 % 4, index // 2 % 4, index % 2
    env, tm = lax.axis_index("env"), lax.axis_index("tm")
    far_z = (env // 2 + z + 2) % 4
    far_y = (tm // 4 + y + 2) % 4
    far_x = (tm % 4 + x + 2) % 4
    return far_z * 2 + (env % 2 + 1 - core) % 2, far_y * 4 + far_x


def for_each_peer(act):
    own = 2 * 32 + 2 * 8 + 2 * 2 + 1
    lax.fori_loop(0, own, lambda i, c: act(*peers(i)), None)
    lax.fori_loop(own + 1, 128, lambda i, c: act(*peers(i)), None)


def exchange_kernel(shards, message, result, gathered, send_sem, recv_sem):
    devices = gathered.shape[0]
    me = lax.axis_index("env") * shards + lax.axis_index("tm")
    barrier = pltpu.get_barrier_semaphore()

    def greet(env, tm):
        pl.semaphore_signal(barrier, inc=1, device_id=(env, tm), device_id_type=MESH)

    def send(env, tm):
        pltpu.make_async_remote_copy(
            src_ref=message,
            dst_ref=gathered.at[pl.ds(me, 1)],
            send_sem=send_sem,
            recv_sem=recv_sem,
            device_id=(env, tm),
            device_id_type=MESH,
        ).start()

    for_each_peer(greet)
    pl.semaphore_wait(barrier, devices - 1)
    for_each_peer(send)
    gathered[pl.ds(me, 1)] = message[...]
    others = gathered.at[pl.ds(0, devices - 1)]
    pltpu.make_async_copy(others, others, recv_sem).wait()

    fields = gathered[...].reshape(devices, BLOCK).T
    pair = lax.broadcasted_iota(jnp.int32, (8, devices), 0)

    def field(k):
        both = [jnp.broadcast_to(fields[e * FIELDS + k : e * FIELDS + k + 1], (8, devices)) for e in range(2)]
        return jnp.where(pair == 0, both[0], both[1])

    lane = lax.broadcasted_iota(jnp.int32, (8, devices), 1)
    shard = lane % shards
    offset, factor, first, last = field(0), field(1), field(2), field(3)
    following = jnp.where(shard < shards - 1, shifted_left(first, 1), field(10))
    jump = (following - last) * field(9)
    reached = offset + factor * jump
    by = 1
    while by < shards:
        inside = shard + by < shards
        reached = reached + factor * jnp.where(inside, shifted_left(reached, by), 0.0)
        factor = factor * jnp.where(inside, shifted_left(factor, by), 1.0)
        by *= 2
    entering = jump + jnp.where(shard < shards - 1, shifted_left(reached, 1), 0.0)
    mean = field(4) + entering * field(5)
    spread_of = field(6) + entering * (2.0 * field(7) + entering * field(8))
    two = pair < 2

    def over_all(array):
        return jnp.sum(jnp.where(two, array, 0.0), keepdims=True) / (2 * devices)

    adv_mean = over_all(mean)
    off = mean - adv_mean
    adv_var = over_all(spread_of + off * off)
    own = jnp.sum(jnp.where(lane == me, entering, 0.0), axis=1, keepdims=True)
    place = lax.broadcasted_iota(jnp.int32, (2, BLOCK), 1)
    line = jnp.where(place == 0, own[:2], adv_mean)
    result[...] = jnp.where(place == 2, lax.rsqrt(adv_var + 1e-05), line)
    pltpu.make_async_copy(others, others, send_sem).wait()


def on_device(
    observations,
    stored_values,
    rewards,
    episode_ends,
    stale_list,
    discount_horizon,
    trace_horizon,
    bootstrap,
    norm_gain,
    input_weight,
    value_head,
):
    env_rows, steps, features = observations.shape
    slots = env_rows * steps // BLOCK
    width = input_weight.shape[1]
    shape = jax.ShapeDtypeStruct((env_rows, steps), jnp.float32)
    vmem, smem, anywhere = (
        pl.BlockSpec(memory_space=pltpu.VMEM),
        pl.BlockSpec(memory_space=pltpu.SMEM),
        pl.BlockSpec(memory_space=pl.ANY),
    )
    offset, factor, value, message = pl.pallas_call(
        sweep_kernel,
        name="sweep",
        out_shape=(shape, shape, shape, jax.ShapeDtypeStruct((1, 1, BLOCK), jnp.float32)),
        in_specs=[smem] * 4 + [anywhere] * 2 + [vmem] * 5,
        out_specs=[vmem] * 4,
        scratch_shapes=[
            pltpu.VMEM((slots, BLOCK, features), jnp.bfloat16),
            pltpu.VMEM((features, width), jnp.bfloat16),
            pltpu.VMEM((2 * BLOCK, features), jnp.bfloat16),
            pltpu.VMEM((2 * BLOCK, features), jnp.bfloat16),
            pltpu.VMEM((16, BLOCK), jnp.float32),
            pltpu.VMEM((2, 16, BLOCK), jnp.float32),
            pltpu.SemaphoreType.DMA((slots,)),
            pltpu.SemaphoreType.DMA((width // CHUNK,)),
        ],
        compiler_params=pltpu.CompilerParams(vmem_limit_bytes=60 * 1024 * 1024),
    )(
        stale_list,
        discount_horizon,
        trace_horizon,
        bootstrap,
        observations.reshape(slots, BLOCK, features),
        input_weight,
        stored_values,
        rewards,
        episode_ends,
        norm_gain.reshape(1, features),
        value_head.astype(jnp.float32).reshape(1, width),
    )
    devices, shards = lax.axis_size("env") * lax.axis_size("tm"), lax.axis_size("tm")
    joined = pl.pallas_call(
        functools.partial(exchange_kernel, shards),
        name="exchange",
        out_shape=jax.ShapeDtypeStruct((env_rows, BLOCK), jnp.float32),
        in_specs=[vmem],
        out_specs=vmem,
        scratch_shapes=[
            pltpu.VMEM((devices, 1, BLOCK), jnp.float32),
            pltpu.SemaphoreType.DMA,
            pltpu.SemaphoreType.DMA,
        ],
        compiler_params=pltpu.CompilerParams(collective_id=0, has_side_effects=True),
    )(message)
    advantage = offset + factor * joined[:, :1]
    return advantage + value, (advantage - joined[:, 1:2]) * joined[:, 2:3]


def solution(mesh):
    placed = (
        P("env", "tm", None),
        P("env", "tm"),
        P("env", "tm"),
        P("env", "tm"),
        P("env", "tm", None),
        P("env"),
        P("env"),
        P("env"),
        P(),
        P(),
        P(),
    )
    return jax.shard_map(
        on_device,
        mesh=mesh,
        in_specs=placed,
        out_specs=(P("env", "tm"), P("env", "tm")),
        check_vma=False,
    )
```

```python
import functools

import jax
import jax.numpy as jnp
from jax import lax
from jax.experimental import pallas as pl
from jax.experimental.pallas import tpu as pltpu
from jax.sharding import PartitionSpec as P

BLOCK = 128
CHUNK = 512
PIECE = 32
FIELDS = 16
MESH = pl.DeviceIdType.MESH


def spread(pair, rows, half):
    row = lax.broadcasted_iota(jnp.int32, (rows, BLOCK), 0)
    return jnp.where(row < half, pair[0], pair[1])


def shifted_left(value, by):
    return pltpu.roll(value, value.shape[1] - by, 1)


def shifted_up(value, by):
    return pltpu.roll(value, value.shape[0] - by, 0)


def sweep_kernel(
    listed,
    discount_horizon,
    trace_horizon,
    bootstrap,
    obs,
    weight,
    stored,
    rewards,
    ends,
    gain,
    head,
    offset_ref,
    factor_ref,
    value_ref,
    message_ref,
    raw,
    held,
    normed_a,
    normed_b,
    fresh,
    packed,
    half_gain,
    head_rows,
    raw_sem,
    held_sem,
):
    slots, _, features = raw.shape
    width = held.shape[1]
    chunks = width // CHUNK
    env_rows, steps = stored.shape
    per_row = steps // BLOCK
    count = jnp.int32(0)
    for j in range(slots):
        count += (listed[0, 0, j] >= 0).astype(jnp.int32)
    groups = (count + 1) // 2

    def raw_copy(slot):
        block = jnp.maximum(listed[0, 0, slot], 0)
        return pltpu.make_async_copy(obs.at[block], raw.at[slot], raw_sem.at[slot])

    def held_copy(c):
        part = pl.ds(c * CHUNK, CHUNK)
        return pltpu.make_async_copy(
            weight.at[:, part], held.at[:, part], held_sem.at[c]
        )

    def start_raw(slot):
        @pl.when(slot < count)
        def _():
            raw_copy(slot).start()

    def wait_group(group):
        for side in range(2):
            slot = 2 * group + side

            @pl.when(slot < count)
            def _():
                raw_copy(slot).wait()

    def normalize(group, piece, target):
        per_block = BLOCK // PIECE
        slot = jnp.minimum(2 * group + piece // per_block, slots - 1)
        rows = pl.ds((piece % per_block) * PIECE, PIECE)
        widened = raw[slot, rows, :].astype(jnp.float32)
        square_mean = jnp.mean(widened * widened, axis=-1, keepdims=True)
        scaled = widened * lax.rsqrt(square_mean + 1e-05) * half_gain[...]
        target[pl.ds(piece * PIECE, PIECE), :] = scaled.astype(jnp.bfloat16)

    def run_group(group, source, target, may_be_first):
        pieces = 2 * BLOCK // PIECE
        total = jnp.zeros((2 * BLOCK, BLOCK), jnp.float32)
        for c in range(chunks):
            if may_be_first:

                @pl.when(group == 0)
                def _():
                    held_copy(c).wait()

            part = pl.ds(c * CHUNK, CHUNK)
            hidden = jnp.dot(
                source[...], held[:, part], preferred_element_type=jnp.float32
            )
            for k in range(CHUNK // BLOCK):
                here = hidden[:, k * BLOCK : (k + 1) * BLOCK]
                active = (here + here * jnp.tanh(here)).astype(jnp.bfloat16)
                line = c * (CHUNK // BLOCK) + k
                total += active.astype(jnp.float32) * head_rows[line : line + 1, :]
            for piece in range(c * pieces // chunks, (c + 1) * pieces // chunks):
                normalize(group + 1, piece, target)
        for side in range(2):
            slot = 2 * group + side
            scores = jnp.sum(
                total[side * BLOCK : (side + 1) * BLOCK].T, axis=0, keepdims=True
            )

            @pl.when(slot < count)
            def _():
                fresh[pl.ds(listed[0, 0, jnp.minimum(slot, slots - 1)], 1), :] = scores

    for e in range(env_rows):
        for k in range(per_row):
            row, part = pl.ds(e * per_row + k, 1), pl.ds(k * BLOCK, BLOCK)
            fresh[row, :] = stored[e : e + 1, part]
            packed[0, row, :] = rewards[e : e + 1, part]
            packed[1, row, :] = 1.0 - ends[e : e + 1, part].astype(jnp.float32)

    @pl.when(count > 0)
    def _():
        for slot in range(2):
            start_raw(slot)
        for c in range(chunks):
            held_copy(c).start()
            if c == chunks // 2:
                for slot in range(2, 4):
                    start_raw(slot)
        for slot in range(4, slots):
            start_raw(slot)
        half_gain[...] = 0.5 * gain[...]
        head_rows[...] = head[...].astype(jnp.float32)
        wait_group(0)
        for piece in range(2 * BLOCK // PIECE):
            normalize(0, piece, normed_a)

        def two_groups(i, carry):
            wait_group(2 * i + 1)
            run_group(2 * i, normed_a, normed_b, True)

            @pl.when(2 * i + 1 < groups)
            def _():
                wait_group(2 * i + 2)
                run_group(2 * i + 1, normed_b, normed_a, False)

            return carry

        lax.fori_loop(0, (groups + 1) // 2, two_groups, 0)

    rows = fresh.shape[0]
    half = per_row
    value = fresh[...]
    lane = lax.broadcasted_iota(jnp.int32, (rows, BLOCK), 1)
    row = lax.broadcasted_iota(jnp.int32, (rows, BLOCK), 0)
    place = jnp.where(row < half, row, row - half)
    discount = 1.0 - 1.0 / spread((discount_horizon[0], discount_horizon[1]), rows, half)
    trace = 1.0 - 1.0 / spread((trace_horizon[0], trace_horizon[1]), rows, half)
    live = row < env_rows * half
    reward = jnp.where(live, packed[0], 0.0)
    going = jnp.where(live, packed[1], 0.0)
    value = jnp.where(live, value, 0.0)
    turned = shifted_left(value, 1)
    following = jnp.where(lane < BLOCK - 1, turned, shifted_up(turned, 1))
    last = (lane == BLOCK - 1) & (place == half - 1)
    following = jnp.where(last, value, following)
    factor = discount * trace * going
    offset = reward + discount * going * following - value
    by = 1
    while by < BLOCK:
        inside = lane < BLOCK - by
        offset = offset + factor * jnp.where(inside, shifted_left(offset, by), 0.0)
        factor = factor * jnp.where(inside, shifted_left(factor, by), 1.0)
        by *= 2
    row_factor = jnp.broadcast_to(factor[:, :1], (rows, BLOCK))
    row_offset = jnp.broadcast_to(offset[:, :1], (rows, BLOCK))
    by = 1
    while by < half:
        inside = place + by < half
        row_offset = row_offset + row_factor * jnp.where(
            inside, shifted_up(row_offset, by), 0.0
        )
        row_factor = row_factor * jnp.where(inside, shifted_up(row_factor, by), 1.0)
        by *= 2
    inside = place + 1 < half
    offset = offset + factor * jnp.where(inside, shifted_up(row_offset, 1), 0.0)
    factor = factor * jnp.where(inside, shifted_up(row_factor, 1), 1.0)

    packed[0] = offset
    packed[1] = factor
    fresh[...] = value
    lanes = lax.broadcasted_iota(jnp.int32, (1, BLOCK), 1)
    line = jnp.zeros((1, BLOCK), jnp.float32)
    for e in range(env_rows):
        mine = live & (row >= e * half) & (row < (e + 1) * half)

        def mean_of(array):
            return jnp.sum(jnp.where(mine, array, 0.0), keepdims=True) / steps

        mean_offset, mean_factor = mean_of(offset), mean_of(factor)
        near, far = offset - mean_offset, factor - mean_factor
        items = (
            row_offset[e * half : e * half + 1, :1],
            row_factor[e * half : e * half + 1, :1],
            value[e * half : e * half + 1, :1],
            value[(e + 1) * half - 1 : (e + 1) * half, BLOCK - 1 :],
            mean_offset,
            mean_factor,
            mean_of(near * near),
            mean_of(near * far),
            mean_of(far * far),
            1.0 / trace[e * half : e * half + 1, :1],
            jnp.full((1, 1), bootstrap[e], jnp.float32),
        )
        for k, item in enumerate(items):
            line = jnp.where(lanes == e * FIELDS + k, item, line)
        for k in range(per_row):
            source, part = pl.ds(e * per_row + k, 1), pl.ds(k * BLOCK, BLOCK)
            offset_ref[e : e + 1, part] = packed[0, source, :]
            factor_ref[e : e + 1, part] = packed[1, source, :]
            value_ref[e : e + 1, part] = fresh[source, :]
    message_ref[...] = line.reshape(message_ref.shape)


def exchange_kernel(
    shards,
    message,
    offset_ref,
    factor_ref,
    value_ref,
    result,
    gathered,
    partial,
    joined,
    send_sem,
    recv_sem,
    partial_sem,
    joined_sem,
):
    env, tm = lax.axis_index("env"), lax.axis_index("tm")
    envs = joined.shape[0]
    barrier = pltpu.get_barrier_semaphore()

    def each_shard(act):
        def one(i, carry):
            act(env, (tm + shards // 2 + i) % shards)
            return carry

        lax.fori_loop(0, shards // 2, one, 0)
        lax.fori_loop(shards // 2 + 1, shards, one, 0)

    def each_env(act):
        def one(i, carry):
            act((env + envs // 2 + i) % envs, tm)
            return carry

        lax.fori_loop(0, envs // 2, one, 0)
        lax.fori_loop(envs // 2 + 1, envs, one, 0)

    def greet(to_env, to_tm):
        pl.semaphore_signal(
            barrier, inc=1, device_id=(to_env, to_tm), device_id_type=MESH
        )

    def send(source, target, own, start_sem, end_sem):
        def act(to_env, to_tm):
            pltpu.make_async_remote_copy(
                src_ref=source,
                dst_ref=target.at[pl.ds(own, 1)],
                send_sem=start_sem,
                recv_sem=end_sem,
                device_id=(to_env, to_tm),
                device_id_type=MESH,
            ).start()

        return act

    def settle(target, length, sem):
        part = target.at[pl.ds(0, length)]
        pltpu.make_async_copy(part, part, sem).wait()

    gathered[...] = jnp.zeros_like(gathered)
    each_shard(greet)
    each_env(greet)
    pl.semaphore_wait(barrier, shards + envs - 2)
    each_shard(send(message, gathered, tm, send_sem, recv_sem))
    gathered[pl.ds(tm, 1)] = message[...]
    settle(gathered, shards - 1, recv_sem)

    fields = gathered[...].reshape(BLOCK, BLOCK).T
    pair = lax.broadcasted_iota(jnp.int32, (8, BLOCK), 0)
    lane = lax.broadcasted_iota(jnp.int32, (8, BLOCK), 1)

    def field(k):
        first = jnp.broadcast_to(fields[k : k + 1], (8, BLOCK))
        second = jnp.broadcast_to(fields[FIELDS + k : FIELDS + k + 1], (8, BLOCK))
        return jnp.where(pair == 0, first, second)

    offset, factor, last = field(0), field(1), field(3)
    following = jnp.where(lane < shards - 1, shifted_left(field(2), 1), field(10))
    jump = (following - last) * field(9)
    reached = offset + factor * jump
    by = 1
    while by < shards:
        inside = lane + by < shards
        reached = reached + factor * jnp.where(inside, shifted_left(reached, by), 0.0)
        factor = factor * jnp.where(inside, shifted_left(factor, by), 1.0)
        by *= 2
    entering = jump + jnp.where(lane < shards - 1, shifted_left(reached, 1), 0.0)
    mean = field(4) + entering * field(5)
    inner = field(6) + entering * (2.0 * field(7) + entering * field(8))
    counted = (pair < 2) & (lane < shards)

    def over_rows(array):
        return jnp.sum(jnp.where(counted, array, 0.0), keepdims=True) / (2 * shards)

    env_mean = over_rows(mean)
    off = mean - env_mean
    env_var = over_rows(inner + off * off)
    place = lax.broadcasted_iota(jnp.int32, (1, BLOCK), 1)
    line = jnp.where(place == 0, env_mean, jnp.where(place == 1, env_var, 0.0))
    partial[...] = line.reshape(partial.shape)
    own = jnp.sum(jnp.where(lane == tm, entering, 0.0), axis=1, keepdims=True)
    advantage = offset_ref[...] + factor_ref[...] * own[:2]
    result[0] = advantage + value_ref[...]
    each_env(send(partial, joined, env, partial_sem, joined_sem))
    joined[pl.ds(env, 1)] = partial[...]
    settle(joined, envs - 1, joined_sem)

    both = joined[...].reshape(envs, BLOCK)
    means, spans = both[:, :1], both[:, 1:2]
    adv_mean = jnp.sum(means, keepdims=True) / envs
    away = means - adv_mean
    adv_var = jnp.sum(spans + away * away, keepdims=True) / envs
    result[1] = (advantage - adv_mean) * lax.rsqrt(adv_var + 1e-05)
    settle(gathered, shards - 1, send_sem)
    settle(joined, envs - 1, partial_sem)


def on_device(
    observations,
    stored_values,
    rewards,
    episode_ends,
    stale_list,
    discount_horizon,
    trace_horizon,
    bootstrap,
    norm_gain,
    input_weight,
    value_head,
):
    env_rows, steps, features = observations.shape
    slots = env_rows * steps // BLOCK
    width = input_weight.shape[1]
    shape = jax.ShapeDtypeStruct((env_rows, steps), jnp.float32)
    vmem, smem, anywhere = (
        pl.BlockSpec(memory_space=pltpu.VMEM),
        pl.BlockSpec(memory_space=pltpu.SMEM),
        pl.BlockSpec(memory_space=pltpu.HBM),
    )
    offset, factor, value, message = pl.pallas_call(
        sweep_kernel,
        name="sweep",
        out_shape=(shape, shape, shape, jax.ShapeDtypeStruct((1, 1, BLOCK), jnp.float32)),
        in_specs=[smem] * 4 + [anywhere] * 2 + [vmem] * 5,
        out_specs=[vmem] * 4,
        scratch_shapes=[
            pltpu.VMEM((slots, BLOCK, features), jnp.bfloat16),
            pltpu.VMEM((features, width), jnp.bfloat16),
            pltpu.VMEM((2 * BLOCK, features), jnp.bfloat16),
            pltpu.VMEM((2 * BLOCK, features), jnp.bfloat16),
            pltpu.VMEM((16, BLOCK), jnp.float32),
            pltpu.VMEM((2, 16, BLOCK), jnp.float32),
            pltpu.VMEM((1, features), jnp.float32),
            pltpu.VMEM((width // BLOCK, BLOCK), jnp.float32),
            pltpu.SemaphoreType.DMA((slots,)),
            pltpu.SemaphoreType.DMA((width // CHUNK,)),
        ],
        compiler_params=pltpu.CompilerParams(vmem_limit_bytes=59 * 1024 * 1024),
    )(
        stale_list,
        discount_horizon,
        trace_horizon,
        bootstrap,
        observations.reshape(slots, BLOCK, features),
        input_weight,
        stored_values,
        rewards,
        episode_ends,
        norm_gain.reshape(1, features),
        value_head.reshape(width // BLOCK, BLOCK),
    )
    envs, shards = lax.axis_size("env"), lax.axis_size("tm")
    joined = pl.pallas_call(
        functools.partial(exchange_kernel, shards),
        name="exchange",
        out_shape=jax.ShapeDtypeStruct((2, env_rows, steps), jnp.float32),
        in_specs=[vmem] * 4,
        out_specs=vmem,
        scratch_shapes=[
            pltpu.VMEM((BLOCK, 1, BLOCK), jnp.float32),
            pltpu.VMEM((1, 1, BLOCK), jnp.float32),
            pltpu.VMEM((envs, 1, BLOCK), jnp.float32),
        ]
        + [pltpu.SemaphoreType.DMA] * 4,
        compiler_params=pltpu.CompilerParams(
            collective_id=0, has_side_effects=True, vmem_limit_bytes=4 * 1024 * 1024
        ),
    )(message, offset, factor, value)
    return joined[0], joined[1]


def solution(mesh):
    placed = (
        P("env", "tm", None),
        P("env", "tm"),
        P("env", "tm"),
        P("env", "tm"),
        P("env", "tm", None),
        P("env"),
        P("env"),
        P("env"),
        P(),
        P(),
        P(),
    )
    return jax.shard_map(
        on_device,
        mesh=mesh,
        in_specs=placed,
        out_specs=(P("env", "tm"), P("env", "tm")),
        check_vma=False,
    )
```

```python
import functools

import jax
import jax.numpy as jnp
from jax import lax
from jax.experimental import pallas as pl
from jax.experimental.pallas import tpu as pltpu
from jax.sharding import PartitionSpec as P

BLOCK = 128
CHUNK = 512
PIECE = 32
FIELDS = 16
ROWS = 16
SWAP_LIMIT = 4 * 1024 * 1024
CRITIC_LIMIT = 36 * 1024 * 1024
EXCHANGE_LIMIT = 59 * 1024 * 1024
MESH = pl.DeviceIdType.MESH


def spread(pair, rows, half):
    row = lax.broadcasted_iota(jnp.int32, (rows, BLOCK), 0)
    return jnp.where(row < half, pair[0], pair[1])


def partner_of(env):
    return env + 1 - 2 * (env % 2)


def shifted_left(value, by):
    return pltpu.roll(value, value.shape[1] - by, 1)


def shifted_up(value, by):
    return pltpu.roll(value, value.shape[0] - by, 0)


def swap_kernel(
    obs, listed, weight, lent, their_list, held, send_sems, recv_sems, held_sems
):
    chunk = weight.shape[0] // held_sems.shape[0]
    loads = []
    for k in range(held_sems.shape[0]):
        part = pl.ds(k * chunk, chunk)
        loads.append(
            pltpu.make_async_copy(weight.at[part], held.at[part], held_sems.at[k])
        )
    env, tm = lax.axis_index("env"), lax.axis_index("tm")
    partner = partner_of(env)
    barrier = pltpu.get_barrier_semaphore()
    pl.semaphore_signal(barrier, inc=1, device_id=(partner, tm), device_id_type=MESH)
    pl.semaphore_wait(barrier, 1)
    pieces = lent.shape[0]
    kept = obs.shape[0] - pieces

    def remote(source, target, k):
        return pltpu.make_async_remote_copy(
            src_ref=source,
            dst_ref=target,
            send_sem=send_sems.at[k],
            recv_sem=recv_sems.at[k],
            device_id=(partner, tm),
            device_id_type=MESH,
        )

    copies = [remote(listed, their_list, pieces)]
    for k in range(pieces):
        copies.append(remote(obs.at[kept + k], lent.at[k], k))
    for copy in copies:
        copy.start()
    for load in loads:
        load.start()
    for load in loads:
        load.wait()
    for copy in copies:
        copy.wait()


def critic_kernel(
    listed,
    their_list,
    obs,
    lent,
    weight,
    stored,
    rewards,
    ends,
    gain,
    head,
    board,
    raw,
    normed_a,
    normed_b,
    half_gain,
    head_rows,
    flags,
    plan,
    raw_sem,
):
    slots, _, features = raw.shape
    chunks = weight.shape[1] // CHUNK
    env_rows, steps = stored.shape
    per_row = steps // BLOCK
    kept = slots - lent.shape[0]

    def read_list(source, own):
        for p in range(slots):
            flags[own, p] = 0
        total = jnp.int32(0)
        for j in range(slots):
            block = source[0, 0, j]
            total += (block >= 0).astype(jnp.int32)

            @pl.when(block >= 0)
            def _():
                flags[own, block] = 1

        movable = jnp.int32(0)
        for p in range(kept, slots):
            movable += flags[own, p]
        return total, movable

    mine, mine_movable = read_list(listed, 0)
    theirs, theirs_movable = read_list(their_list, 1)
    given = jnp.minimum(jnp.maximum((mine - theirs) // 2, 0), mine_movable)
    taken = jnp.minimum(jnp.maximum((theirs - mine) // 2, 0), theirs_movable)
    count = jnp.int32(0)
    for p in reversed(range(slots)):
        flag = flags[0, p]
        moves = flag * (given > 0).astype(jnp.int32)
        given -= moves
        plan[count] = p
        count += flag - moves
    for p in reversed(range(kept, slots)):
        moves = flags[1, p] * (taken > 0).astype(jnp.int32)
        taken -= moves
        plan[count] = ROWS + p
        count += moves
    groups = (count + 1) // 2

    def raw_copy(slot, act):
        entry = plan[slot]

        @pl.when((slot < count) & (entry < ROWS))
        def _():
            act(pltpu.make_async_copy(obs.at[entry], raw.at[slot], raw_sem.at[slot]))

        @pl.when((slot < count) & (entry >= ROWS))
        def _():
            block = entry - ROWS - kept
            act(pltpu.make_async_copy(lent.at[block], raw.at[slot], raw_sem.at[slot]))

    def wait_group(group):
        for side in range(2):
            raw_copy(2 * group + side, lambda copy: copy.wait())

    def normalize(group, piece, target):
        per_block = BLOCK // PIECE
        slot = jnp.minimum(2 * group + piece // per_block, slots - 1)
        rows = pl.ds((piece % per_block) * PIECE, PIECE)
        widened = raw[slot, rows, :].astype(jnp.float32)
        square_mean = jnp.mean(widened * widened, axis=-1, keepdims=True)
        scaled = widened * lax.rsqrt(square_mean + 1e-05) * half_gain[...]
        target[pl.ds(piece * PIECE, PIECE), :] = scaled.astype(jnp.bfloat16)

    def run_group(group, source, target):
        pieces = 2 * BLOCK // PIECE
        total = jnp.zeros((2 * BLOCK, BLOCK), jnp.float32)
        for c in range(chunks):
            part = pl.ds(c * CHUNK, CHUNK)
            hidden = jnp.dot(
                source[...], weight[:, part], preferred_element_type=jnp.float32
            )
            for k in range(CHUNK // BLOCK):
                here = hidden[:, k * BLOCK : (k + 1) * BLOCK]
                active = (here + here * jnp.tanh(here)).astype(jnp.bfloat16)
                line = c * (CHUNK // BLOCK) + k
                total += active.astype(jnp.float32) * head_rows[line : line + 1, :]
            for piece in range(c * pieces // chunks, (c + 1) * pieces // chunks):
                normalize(group + 1, piece, target)
        for side in range(2):
            slot = 2 * group + side
            scores = jnp.sum(
                total[side * BLOCK : (side + 1) * BLOCK].T, axis=0, keepdims=True
            )
            entry = plan[slot]

            @pl.when((slot < count) & (entry < ROWS))
            def _():
                board[0, pl.ds(entry, 1), :] = scores

            @pl.when((slot < count) & (entry >= ROWS))
            def _():
                board[3, pl.ds(entry - ROWS, 1), :] = scores

    for slot in range(slots):
        raw_copy(slot, lambda copy: copy.start())
    board[...] = jnp.zeros_like(board)
    for e in range(env_rows):
        for k in range(per_row):
            block, part = e * per_row + k, pl.ds(k * BLOCK, BLOCK)
            row = pl.ds(block, 1)
            board[0, row, :] = jnp.where(
                flags[0, block] > 0, 0.0, stored[e : e + 1, part]
            )
            board[1, row, :] = rewards[e : e + 1, part]
            board[2, row, :] = 1.0 - ends[e : e + 1, part].astype(jnp.float32)

    @pl.when(count > 0)
    def _():
        half_gain[...] = 0.5 * gain[...]
        head_rows[...] = head[...].astype(jnp.float32)
        wait_group(0)
        for piece in range(2 * BLOCK // PIECE):
            normalize(0, piece, normed_a)

        def two_groups(i, carry):
            wait_group(2 * i + 1)
            run_group(2 * i, normed_a, normed_b)

            @pl.when(2 * i + 1 < groups)
            def _():
                wait_group(2 * i + 2)
                run_group(2 * i + 1, normed_b, normed_a)

            return carry

        lax.fori_loop(0, (groups + 1) // 2, two_groups, 0)


def exchange_kernel(
    shards,
    discount_horizon,
    trace_horizon,
    bootstrap,
    board,
    result,
    held,
    returned,
    message,
    gathered,
    partial,
    joined,
    send_sem,
    recv_sem,
    partial_sem,
    joined_sem,
    board_sem,
    lend_sem,
    return_sem,
):
    env, tm = lax.axis_index("env"), lax.axis_index("tm")
    envs = joined.shape[0]
    barrier = pltpu.get_barrier_semaphore()

    def each_shard(act):
        def one(i, carry):
            act(env, (tm + shards // 2 + i) % shards)
            return carry

        lax.fori_loop(0, shards // 2, one, 0)
        lax.fori_loop(shards // 2 + 1, shards, one, 0)

    def each_env(act):
        def one(i, carry):
            act((env + envs // 2 + i) % envs, tm)
            return carry

        lax.fori_loop(0, envs // 2, one, 0)
        lax.fori_loop(envs // 2 + 1, envs, one, 0)

    def greet(to_env, to_tm):
        pl.semaphore_signal(
            barrier, inc=1, device_id=(to_env, to_tm), device_id_type=MESH
        )

    def send(source, target, own, start_sem, end_sem):
        def act(to_env, to_tm):
            pltpu.make_async_remote_copy(
                src_ref=source,
                dst_ref=target.at[pl.ds(own, 1)],
                send_sem=start_sem,
                recv_sem=end_sem,
                device_id=(to_env, to_tm),
                device_id_type=MESH,
            ).start()

        return act

    def settle(target, length, sem):
        part = target.at[pl.ds(0, length)]
        pltpu.make_async_copy(part, part, sem).wait()

    load = pltpu.make_async_copy(board, held, board_sem)
    load.start()
    gathered[...] = jnp.zeros_like(gathered)
    each_shard(greet)
    each_env(greet)
    pl.semaphore_wait(barrier, shards + envs - 2)
    load.wait()
    give_back = pltpu.make_async_remote_copy(
        src_ref=held.at[3],
        dst_ref=returned,
        send_sem=lend_sem,
        recv_sem=return_sem,
        device_id=(partner_of(env), tm),
        device_id_type=MESH,
    )
    give_back.start()
    give_back.wait()

    env_rows, steps = result.shape[1:]
    rows, half = ROWS, steps // BLOCK
    value = held[0] + returned[...]
    lane = lax.broadcasted_iota(jnp.int32, (rows, BLOCK), 1)
    row = lax.broadcasted_iota(jnp.int32, (rows, BLOCK), 0)
    place = jnp.where(row < half, row, row - half)
    discount = 1.0 - 1.0 / spread((discount_horizon[0], discount_horizon[1]), rows, half)
    trace = 1.0 - 1.0 / spread((trace_horizon[0], trace_horizon[1]), rows, half)
    live = row < env_rows * half
    reward = held[1]
    going = held[2]
    turned = shifted_left(value, 1)
    following = jnp.where(lane < BLOCK - 1, turned, shifted_up(turned, 1))
    last = (lane == BLOCK - 1) & (place == half - 1)
    following = jnp.where(last, value, following)
    factor = discount * trace * going
    offset = reward + discount * going * following - value
    by = 1
    while by < BLOCK:
        inside = lane < BLOCK - by
        offset = offset + factor * jnp.where(inside, shifted_left(offset, by), 0.0)
        factor = factor * jnp.where(inside, shifted_left(factor, by), 1.0)
        by *= 2
    row_factor = jnp.broadcast_to(factor[:, :1], (rows, BLOCK))
    row_offset = jnp.broadcast_to(offset[:, :1], (rows, BLOCK))
    by = 1
    while by < half:
        inside = place + by < half
        row_offset = row_offset + row_factor * jnp.where(
            inside, shifted_up(row_offset, by), 0.0
        )
        row_factor = row_factor * jnp.where(inside, shifted_up(row_factor, by), 1.0)
        by *= 2
    inside = place + 1 < half
    offset = offset + factor * jnp.where(inside, shifted_up(row_offset, 1), 0.0)
    factor = factor * jnp.where(inside, shifted_up(row_factor, 1), 1.0)
    lanes = lax.broadcasted_iota(jnp.int32, (1, BLOCK), 1)
    line = jnp.zeros((1, BLOCK), jnp.float32)
    for e in range(env_rows):
        mine = live & (row >= e * half) & (row < (e + 1) * half)

        def mean_of(array):
            return jnp.sum(jnp.where(mine, array, 0.0), keepdims=True) / steps

        mean_offset, mean_factor = mean_of(offset), mean_of(factor)
        near, far = offset - mean_offset, factor - mean_factor
        items = (
            row_offset[e * half : e * half + 1, :1],
            row_factor[e * half : e * half + 1, :1],
            value[e * half : e * half + 1, :1],
            value[(e + 1) * half - 1 : (e + 1) * half, BLOCK - 1 :],
            mean_offset,
            mean_factor,
            mean_of(near * near),
            mean_of(near * far),
            mean_of(far * far),
            1.0 / trace[e * half : e * half + 1, :1],
            jnp.full((1, 1), bootstrap[e], jnp.float32),
        )
        for k, item in enumerate(items):
            line = jnp.where(lanes == e * FIELDS + k, item, line)
    message[...] = line.reshape(message.shape)
    each_shard(send(message, gathered, tm, send_sem, recv_sem))
    gathered[pl.ds(tm, 1)] = message[...]
    settle(gathered, shards - 1, recv_sem)

    fields = gathered[...].reshape(BLOCK, BLOCK).T
    pair = lax.broadcasted_iota(jnp.int32, (8, BLOCK), 0)
    spot = lax.broadcasted_iota(jnp.int32, (8, BLOCK), 1)

    def field(k):
        first = jnp.broadcast_to(fields[k : k + 1], (8, BLOCK))
        second = jnp.broadcast_to(fields[FIELDS + k : FIELDS + k + 1], (8, BLOCK))
        return jnp.where(pair == 0, first, second)

    start, scale, end = field(0), field(1), field(3)
    following = jnp.where(spot < shards - 1, shifted_left(field(2), 1), field(10))
    jump = (following - end) * field(9)
    reached = start + scale * jump
    by = 1
    while by < shards:
        inside = spot + by < shards
        reached = reached + scale * jnp.where(inside, shifted_left(reached, by), 0.0)
        scale = scale * jnp.where(inside, shifted_left(scale, by), 1.0)
        by *= 2
    entering = jump + jnp.where(spot < shards - 1, shifted_left(reached, 1), 0.0)
    mean = field(4) + entering * field(5)
    inner = field(6) + entering * (2.0 * field(7) + entering * field(8))
    counted = (pair < 2) & (spot < shards)

    def over_rows(array):
        return jnp.sum(jnp.where(counted, array, 0.0), keepdims=True) / (2 * shards)

    env_mean = over_rows(mean)
    off = mean - env_mean
    env_var = over_rows(inner + off * off)
    place = lax.broadcasted_iota(jnp.int32, (1, BLOCK), 1)
    line = jnp.where(place == 0, env_mean, jnp.where(place == 1, env_var, 0.0))
    partial[...] = line.reshape(partial.shape)
    own = jnp.sum(jnp.where(spot == tm, entering, 0.0), axis=1, keepdims=True)
    advantage = offset + factor * jnp.where(row < half, own[:1], own[1:2])

    def put(which, array):
        for e in range(env_rows):
            for k in range(half):
                line = e * half + k
                result[which, e : e + 1, pl.ds(k * BLOCK, BLOCK)] = array[line : line + 1]

    put(0, advantage + value)
    each_env(send(partial, joined, env, partial_sem, joined_sem))
    joined[pl.ds(env, 1)] = partial[...]
    settle(joined, envs - 1, joined_sem)

    both = joined[...].reshape(envs, BLOCK)
    means, spans = both[:, :1], both[:, 1:2]
    adv_mean = jnp.sum(means, keepdims=True) / envs
    away = means - adv_mean
    adv_var = jnp.sum(spans + away * away, keepdims=True) / envs
    put(1, (advantage - adv_mean) * lax.rsqrt(adv_var + 1e-05))
    settle(gathered, shards - 1, send_sem)
    settle(joined, envs - 1, partial_sem)


def on_device(
    observations,
    stored_values,
    rewards,
    episode_ends,
    stale_list,
    discount_horizon,
    trace_horizon,
    bootstrap,
    norm_gain,
    input_weight,
    value_head,
):
    env_rows, steps, features = observations.shape
    slots = env_rows * steps // BLOCK
    width = input_weight.shape[1]
    lent_blocks = slots // 2
    blocks = observations.reshape(slots, BLOCK, features)
    in_space = pltpu.with_memory_space_constraint
    blocks = in_space(blocks, pltpu.HBM)
    listed = in_space(stale_list, pltpu.HBM)
    weight = in_space(input_weight, pltpu.HBM)
    vmem, smem, hbm = (
        pl.BlockSpec(memory_space=space) for space in (pltpu.VMEM, pltpu.SMEM, pltpu.HBM)
    )
    lent, their_list, held = pl.pallas_call(
        swap_kernel,
        name="swap",
        out_shape=(
            pltpu.VMEM((lent_blocks, BLOCK, features), observations.dtype),
            pltpu.HBM(stale_list.shape, stale_list.dtype),
            pltpu.VMEM(input_weight.shape, input_weight.dtype),
        ),
        in_specs=[hbm] * 3,
        out_specs=[vmem, hbm, vmem],
        scratch_shapes=[
            pltpu.SemaphoreType.DMA((lent_blocks + 1,)),
            pltpu.SemaphoreType.DMA((lent_blocks + 1,)),
            pltpu.SemaphoreType.DMA((4,)),
        ],
        compiler_params=pltpu.CompilerParams(
            collective_id=1, has_side_effects=True, vmem_limit_bytes=SWAP_LIMIT
        ),
    )(blocks, listed, weight)
    board = pl.pallas_call(
        critic_kernel,
        name="critic",
        out_shape=jax.ShapeDtypeStruct((4, ROWS, BLOCK), jnp.float32),
        in_specs=[smem] * 2 + [hbm] + [vmem] * 7,
        out_specs=vmem,
        scratch_shapes=[
            pltpu.VMEM((slots, BLOCK, features), jnp.bfloat16),
            pltpu.VMEM((2 * BLOCK, features), jnp.bfloat16),
            pltpu.VMEM((2 * BLOCK, features), jnp.bfloat16),
            pltpu.VMEM((1, features), jnp.float32),
            pltpu.VMEM((width // BLOCK, BLOCK), jnp.float32),
            pltpu.SMEM((2, ROWS), jnp.int32),
            pltpu.SMEM((2 * ROWS,), jnp.int32),
            pltpu.SemaphoreType.DMA((slots,)),
        ],
        compiler_params=pltpu.CompilerParams(vmem_limit_bytes=CRITIC_LIMIT),
    )(
        stale_list,
        in_space(their_list, pltpu.HBM),
        blocks,
        in_space(lent, pltpu.VMEM),
        in_space(held, pltpu.VMEM),
        stored_values,
        rewards,
        episode_ends,
        norm_gain.reshape(1, features),
        value_head.reshape(width // BLOCK, BLOCK),
    )
    envs, shards = lax.axis_size("env"), lax.axis_size("tm")
    joined = pl.pallas_call(
        functools.partial(exchange_kernel, shards),
        name="exchange",
        out_shape=jax.ShapeDtypeStruct((2, env_rows, steps), jnp.float32),
        in_specs=[smem] * 3 + [hbm],
        out_specs=vmem,
        scratch_shapes=[
            pltpu.VMEM((4, ROWS, BLOCK), jnp.float32),
            pltpu.VMEM((ROWS, BLOCK), jnp.float32),
            pltpu.VMEM((1, 1, BLOCK), jnp.float32),
            pltpu.VMEM((BLOCK, 1, BLOCK), jnp.float32),
            pltpu.VMEM((1, 1, BLOCK), jnp.float32),
            pltpu.VMEM((envs, 1, BLOCK), jnp.float32),
        ]
        + [pltpu.SemaphoreType.DMA] * 7,
        compiler_params=pltpu.CompilerParams(
            collective_id=0, has_side_effects=True, vmem_limit_bytes=EXCHANGE_LIMIT
        ),
    )(discount_horizon, trace_horizon, bootstrap, board)
    return joined[0], joined[1]


def solution(mesh):
    placed = (
        P("env", "tm", None),
        P("env", "tm"),
        P("env", "tm"),
        P("env", "tm"),
        P("env", "tm", None),
        P("env"),
        P("env"),
        P("env"),
        P(),
        P(),
        P(),
    )
    return jax.shard_map(
        on_device,
        mesh=mesh,
        in_specs=placed,
        out_specs=(P("env", "tm"), P("env", "tm")),
        check_vma=False,
    )
```

```python
import functools

import jax
import jax.numpy as jnp
from jax import lax
from jax.experimental import pallas as pl
from jax.experimental.pallas import tpu as pltpu
from jax.sharding import PartitionSpec as P

BLOCK = 128
CHUNK = 512
PIECE = 32
FIELDS = 16
MESH = pl.DeviceIdType.MESH


def spread(pair, rows, half):
    row = lax.broadcasted_iota(jnp.int32, (rows, BLOCK), 0)
    return jnp.where(row < half, pair[0], pair[1])


def shifted_left(value, by):
    return pltpu.roll(value, value.shape[1] - by, 1)


def shifted_up(value, by):
    return pltpu.roll(value, value.shape[0] - by, 0)


def sweep_kernel(
    listed,
    discount_horizon,
    trace_horizon,
    bootstrap,
    obs,
    weight,
    stored,
    rewards,
    ends,
    gain,
    head,
    offset_ref,
    factor_ref,
    value_ref,
    message_ref,
    raw,
    held,
    normed,
    fresh,
    packed,
    half_gain,
    head_rows,
    raw_sem,
    held_sem,
):
    slots, _, features = raw.shape
    width = held.shape[1]
    chunks = width // CHUNK
    env_rows, steps = stored.shape
    per_row = steps // BLOCK
    count = jnp.int32(0)
    for j in range(slots):
        count += (listed[0, 0, j] >= 0).astype(jnp.int32)
    groups = (count + 1) // 2

    def raw_copy(slot):
        block = jnp.maximum(listed[0, 0, slot], 0)
        return pltpu.make_async_copy(obs.at[block], raw.at[slot], raw_sem.at[slot])

    def held_copy(c):
        part = pl.ds(c * CHUNK, CHUNK)
        return pltpu.make_async_copy(
            weight.at[:, part], held.at[:, part], held_sem.at[c]
        )

    def start_raw(slot):
        @pl.when(slot < count)
        def _():
            raw_copy(slot).start()

    def wait_raw(slot):
        @pl.when(slot < count)
        def _():
            raw_copy(slot).wait()

    def normalize(start, length):
        rows = pl.ds(start, length)
        widened = raw[start // BLOCK, pl.ds(start % BLOCK, length), :].astype(jnp.float32)
        square_mean = jnp.mean(widened * widened, axis=-1, keepdims=True)
        scaled = widened * lax.rsqrt(square_mean + 1e-05) * half_gain[...]
        normed[rows, :] = scaled.astype(jnp.bfloat16)

    def run_group(group, first):
        rows = pl.ds(0, 2 * BLOCK)
        if not first:
            rows = pl.ds(pl.multiple_of(group * (2 * BLOCK), 2 * BLOCK), 2 * BLOCK)
        total = jnp.zeros((2 * BLOCK, BLOCK), jnp.float32)
        ready = 2
        for c in range(chunks):
            if first:
                held_copy(c).wait()
                bound = 2 + (c + 1) * (slots - 2) // chunks
                for slot in range(ready, bound):
                    wait_raw(slot)
            part = pl.ds(c * CHUNK, CHUNK)
            hidden = jnp.dot(
                normed[rows, :], held[:, part], preferred_element_type=jnp.float32
            )
            for k in range(CHUNK // BLOCK):
                here = hidden[:, k * BLOCK : (k + 1) * BLOCK]
                active = (here + here * jnp.tanh(here)).astype(jnp.bfloat16)
                line = c * (CHUNK // BLOCK) + k
                total += active.astype(jnp.float32) * head_rows[line : line + 1, :]
            if first:
                for start in range(ready * BLOCK, bound * BLOCK, PIECE):
                    normalize(start, PIECE)
                ready = bound
        for side in range(2):
            slot = 2 * group + side
            scores = jnp.sum(
                total[side * BLOCK : (side + 1) * BLOCK].T, axis=0, keepdims=True
            )

            @pl.when(slot < count)
            def _():
                fresh[pl.ds(listed[0, 0, slot], 1), :] = scores

    @pl.when(count > 0)
    def _():
        for slot in range(2):
            start_raw(slot)
        after = 2
        for c in range(chunks):
            held_copy(c).start()
            bound = 2 + (c + 1) * (slots - 2) // chunks
            for slot in range(after, bound):
                start_raw(slot)
            after = bound

    for e in range(env_rows):
        for k in range(per_row):
            row, part = pl.ds(e * per_row + k, 1), pl.ds(k * BLOCK, BLOCK)
            fresh[row, :] = stored[e : e + 1, part]
            packed[0, row, :] = rewards[e : e + 1, part]
            packed[1, row, :] = 1.0 - ends[e : e + 1, part].astype(jnp.float32)

    @pl.when(count > 0)
    def _():
        half_gain[...] = 0.5 * gain[...]
        head_rows[...] = head[...].astype(jnp.float32)
        for slot in range(2):
            wait_raw(slot)
        for start in range(0, 2 * BLOCK, PIECE):
            normalize(start, PIECE)
        run_group(0, True)

        def one_group(i, carry):
            run_group(i, False)
            return carry

        lax.fori_loop(1, groups, one_group, 0)

    rows = fresh.shape[0]
    half = per_row
    value = fresh[...]
    lane = lax.broadcasted_iota(jnp.int32, (rows, BLOCK), 1)
    row = lax.broadcasted_iota(jnp.int32, (rows, BLOCK), 0)
    place = jnp.where(row < half, row, row - half)
    discount = 1.0 - 1.0 / spread((discount_horizon[0], discount_horizon[1]), rows, half)
    trace = 1.0 - 1.0 / spread((trace_horizon[0], trace_horizon[1]), rows, half)
    live = row < env_rows * half
    reward = jnp.where(live, packed[0], 0.0)
    going = jnp.where(live, packed[1], 0.0)
    value = jnp.where(live, value, 0.0)
    turned = shifted_left(value, 1)
    following = jnp.where(lane < BLOCK - 1, turned, shifted_up(turned, 1))
    last = (lane == BLOCK - 1) & (place == half - 1)
    following = jnp.where(last, value, following)
    factor = discount * trace * going
    offset = reward + discount * going * following - value
    by = 1
    while by < BLOCK:
        inside = lane < BLOCK - by
        offset = offset + factor * jnp.where(inside, shifted_left(offset, by), 0.0)
        factor = factor * jnp.where(inside, shifted_left(factor, by), 1.0)
        by *= 2
    row_factor = jnp.broadcast_to(factor[:, :1], (rows, BLOCK))
    row_offset = jnp.broadcast_to(offset[:, :1], (rows, BLOCK))
    by = 1
    while by < half:
        inside = place + by < half
        row_offset = row_offset + row_factor * jnp.where(
            inside, shifted_up(row_offset, by), 0.0
        )
        row_factor = row_factor * jnp.where(inside, shifted_up(row_factor, by), 1.0)
        by *= 2
    inside = place + 1 < half
    offset = offset + factor * jnp.where(inside, shifted_up(row_offset, 1), 0.0)
    factor = factor * jnp.where(inside, shifted_up(row_factor, 1), 1.0)

    packed[0] = offset
    packed[1] = factor
    fresh[...] = value
    lanes = lax.broadcasted_iota(jnp.int32, (1, BLOCK), 1)
    line = jnp.zeros((1, BLOCK), jnp.float32)
    for e in range(env_rows):
        mine = live & (row >= e * half) & (row < (e + 1) * half)

        def mean_of(array):
            return jnp.sum(jnp.where(mine, array, 0.0), keepdims=True) / steps

        mean_offset, mean_factor = mean_of(offset), mean_of(factor)
        near, far = offset - mean_offset, factor - mean_factor
        items = (
            row_offset[e * half : e * half + 1, :1],
            row_factor[e * half : e * half + 1, :1],
            value[e * half : e * half + 1, :1],
            value[(e + 1) * half - 1 : (e + 1) * half, BLOCK - 1 :],
            mean_offset,
            mean_factor,
            mean_of(near * near),
            mean_of(near * far),
            mean_of(far * far),
            1.0 / trace[e * half : e * half + 1, :1],
            jnp.full((1, 1), bootstrap[e], jnp.float32),
        )
        for k, item in enumerate(items):
            line = jnp.where(lanes == e * FIELDS + k, item, line)
        for k in range(per_row):
            source, part = pl.ds(e * per_row + k, 1), pl.ds(k * BLOCK, BLOCK)
            offset_ref[e : e + 1, part] = packed[0, source, :]
            factor_ref[e : e + 1, part] = packed[1, source, :]
            value_ref[e : e + 1, part] = fresh[source, :]
    message_ref[...] = line.reshape(message_ref.shape)


def exchange_kernel(
    shards,
    message,
    offset_ref,
    factor_ref,
    value_ref,
    result,
    gathered,
    partial,
    joined,
    send_sem,
    recv_sem,
    partial_sem,
    joined_sem,
):
    env, tm = lax.axis_index("env"), lax.axis_index("tm")
    envs = joined.shape[0]
    barrier = pltpu.get_barrier_semaphore()

    def each_shard(act):
        def one(i, carry):
            act(env, (tm + shards // 2 + i) % shards)
            return carry

        lax.fori_loop(0, shards // 2, one, 0)
        lax.fori_loop(shards // 2 + 1, shards, one, 0)

    def each_env(act):
        def one(i, carry):
            act((env + envs // 2 + i) % envs, tm)
            return carry

        lax.fori_loop(0, envs // 2, one, 0)
        lax.fori_loop(envs // 2 + 1, envs, one, 0)

    def greet(to_env, to_tm):
        pl.semaphore_signal(
            barrier, inc=1, device_id=(to_env, to_tm), device_id_type=MESH
        )

    def send(source, target, own, start_sem, end_sem):
        def act(to_env, to_tm):
            pltpu.make_async_remote_copy(
                src_ref=source,
                dst_ref=target.at[pl.ds(own, 1)],
                send_sem=start_sem,
                recv_sem=end_sem,
                device_id=(to_env, to_tm),
                device_id_type=MESH,
            ).start()

        return act

    def settle(target, length, sem):
        part = target.at[pl.ds(0, length)]
        pltpu.make_async_copy(part, part, sem).wait()

    gathered[...] = jnp.zeros_like(gathered)
    each_shard(greet)
    each_env(greet)
    pl.semaphore_wait(barrier, shards + envs - 2)
    each_shard(send(message, gathered, tm, send_sem, recv_sem))
    gathered[pl.ds(tm, 1)] = message[...]
    settle(gathered, shards - 1, recv_sem)

    fields = gathered[...].reshape(BLOCK, BLOCK).T
    pair = lax.broadcasted_iota(jnp.int32, (8, BLOCK), 0)
    lane = lax.broadcasted_iota(jnp.int32, (8, BLOCK), 1)

    def field(k):
        first = jnp.broadcast_to(fields[k : k + 1], (8, BLOCK))
        second = jnp.broadcast_to(fields[FIELDS + k : FIELDS + k + 1], (8, BLOCK))
        return jnp.where(pair == 0, first, second)

    offset, factor, last = field(0), field(1), field(3)
    following = jnp.where(lane < shards - 1, shifted_left(field(2), 1), field(10))
    jump = (following - last) * field(9)
    reached = offset + factor * jump
    by = 1
    while by < shards:
        inside = lane + by < shards
        reached = reached + factor * jnp.where(inside, shifted_left(reached, by), 0.0)
        factor = factor * jnp.where(inside, shifted_left(factor, by), 1.0)
        by *= 2
    entering = jump + jnp.where(lane < shards - 1, shifted_left(reached, 1), 0.0)
    mean = field(4) + entering * field(5)
    inner = field(6) + entering * (2.0 * field(7) + entering * field(8))
    counted = (pair < 2) & (lane < shards)

    def over_rows(array):
        return jnp.sum(jnp.where(counted, array, 0.0), keepdims=True) / (2 * shards)

    env_mean = over_rows(mean)
    off = mean - env_mean
    env_var = over_rows(inner + off * off)
    place = lax.broadcasted_iota(jnp.int32, (1, BLOCK), 1)
    line = jnp.where(place == 0, env_mean, jnp.where(place == 1, env_var, 0.0))
    partial[...] = line.reshape(partial.shape)
    own = jnp.sum(jnp.where(lane == tm, entering, 0.0), axis=1, keepdims=True)
    advantage = offset_ref[...] + factor_ref[...] * own[:2]
    result[0] = advantage + value_ref[...]
    each_env(send(partial, joined, env, partial_sem, joined_sem))
    joined[pl.ds(env, 1)] = partial[...]
    settle(joined, envs - 1, joined_sem)

    both = joined[...].reshape(envs, BLOCK)
    means, spans = both[:, :1], both[:, 1:2]
    adv_mean = jnp.sum(means, keepdims=True) / envs
    away = means - adv_mean
    adv_var = jnp.sum(spans + away * away, keepdims=True) / envs
    result[1] = (advantage - adv_mean) * lax.rsqrt(adv_var + 1e-05)
    settle(gathered, shards - 1, send_sem)
    settle(joined, envs - 1, partial_sem)


def on_device(
    observations,
    stored_values,
    rewards,
    episode_ends,
    stale_list,
    discount_horizon,
    trace_horizon,
    bootstrap,
    norm_gain,
    input_weight,
    value_head,
):
    env_rows, steps, features = observations.shape
    slots = env_rows * steps // BLOCK
    width = input_weight.shape[1]
    shape = pltpu.VMEM((env_rows, steps), jnp.float32)
    in_space = pltpu.with_memory_space_constraint
    vmem, smem, anywhere = (
        pl.BlockSpec(memory_space=pltpu.VMEM),
        pl.BlockSpec(memory_space=pltpu.SMEM),
        pl.BlockSpec(memory_space=pltpu.HBM),
    )
    offset, factor, value, message = pl.pallas_call(
        sweep_kernel,
        name="sweep",
        out_shape=(shape, shape, shape, pltpu.VMEM((1, 1, BLOCK), jnp.float32)),
        in_specs=[smem] * 4 + [anywhere] * 2 + [vmem] * 5,
        out_specs=[vmem] * 4,
        scratch_shapes=[
            pltpu.VMEM((slots, BLOCK, features), jnp.bfloat16),
            pltpu.VMEM((features, width), jnp.bfloat16),
            pltpu.VMEM((slots * BLOCK, features), jnp.bfloat16),
            pltpu.VMEM((16, BLOCK), jnp.float32),
            pltpu.VMEM((2, 16, BLOCK), jnp.float32),
            pltpu.VMEM((1, features), jnp.float32),
            pltpu.VMEM((width // BLOCK, BLOCK), jnp.float32),
            pltpu.SemaphoreType.DMA((slots,)),
            pltpu.SemaphoreType.DMA((width // CHUNK,)),
        ],
        compiler_params=pltpu.CompilerParams(vmem_limit_bytes=57 * 1024 * 1024),
    )(
        stale_list,
        discount_horizon,
        trace_horizon,
        bootstrap,
        in_space(observations.reshape(slots, BLOCK, features), pltpu.HBM),
        in_space(input_weight, pltpu.HBM),
        stored_values,
        rewards,
        episode_ends,
        norm_gain.reshape(1, features),
        value_head.reshape(width // BLOCK, BLOCK),
    )
    envs, shards = lax.axis_size("env"), lax.axis_size("tm")
    joined = pl.pallas_call(
        functools.partial(exchange_kernel, shards),
        name="exchange",
        out_shape=jax.ShapeDtypeStruct((2, env_rows, steps), jnp.float32),
        in_specs=[vmem] * 4,
        out_specs=vmem,
        scratch_shapes=[
            pltpu.VMEM((BLOCK, 1, BLOCK), jnp.float32),
            pltpu.VMEM((1, 1, BLOCK), jnp.float32),
            pltpu.VMEM((envs, 1, BLOCK), jnp.float32),
        ]
        + [pltpu.SemaphoreType.DMA] * 4,
        compiler_params=pltpu.CompilerParams(
            collective_id=0, has_side_effects=True, vmem_limit_bytes=57 * 1024 * 1024
        ),
    )(*(in_space(array, pltpu.VMEM) for array in (message, offset, factor, value)))
    return joined[0], joined[1]


def solution(mesh):
    placed = (
        P("env", "tm", None),
        P("env", "tm"),
        P("env", "tm"),
        P("env", "tm"),
        P("env", "tm", None),
        P("env"),
        P("env"),
        P("env"),
        P(),
        P(),
        P(),
    )
    return jax.shard_map(
        on_device,
        mesh=mesh,
        in_specs=placed,
        out_specs=(P("env", "tm"), P("env", "tm")),
        check_vma=False,
    )
```

```python
import functools

import jax
import jax.numpy as jnp
from jax import lax
from jax.experimental import pallas as pl
from jax.experimental.pallas import tpu as pltpu
from jax.sharding import PartitionSpec as P

BLOCK = 128
CHUNK = 512
PIECE = 32
FIELDS = 16
MESH = pl.DeviceIdType.MESH


def spread(pair, rows, half):
    row = lax.broadcasted_iota(jnp.int32, (rows, BLOCK), 0)
    return jnp.where(row < half, pair[0], pair[1])


def shifted_left(value, by):
    return pltpu.roll(value, value.shape[1] - by, 1)


def shifted_up(value, by):
    return pltpu.roll(value, value.shape[0] - by, 0)


def sweep_kernel(
    listed,
    discount_horizon,
    trace_horizon,
    bootstrap,
    obs,
    weight,
    stored,
    rewards,
    ends,
    gain,
    head,
    offset_ref,
    factor_ref,
    value_ref,
    message_ref,
    raw,
    held,
    normed,
    sums,
    fresh,
    packed,
    half_gain,
    head_rows,
    raw_sem,
    held_sem,
):
    slots, _, features = raw.shape
    width = held.shape[1]
    chunks = width // CHUNK
    env_rows, steps = stored.shape
    per_row = steps // BLOCK
    count = jnp.int32(0)
    for j in range(slots):
        count += (listed[0, 0, j] >= 0).astype(jnp.int32)
    groups = (count + 1) // 2
    lead = (slots - chunks) // 2
    spare = fresh.shape[0] - 1

    def raw_copy(slot):
        block = jnp.maximum(listed[0, 0, slot], 0)
        return pltpu.make_async_copy(obs.at[block], raw.at[slot], raw_sem.at[slot])

    def held_copy(c):
        part = pl.ds(c * CHUNK, CHUNK)
        return pltpu.make_async_copy(
            weight.at[:, part], held.at[:, part], held_sem.at[c]
        )

    def start_raw(slot):
        @pl.when(slot < count)
        def _():
            raw_copy(slot).start()

    def wait_raw(slot):
        @pl.when(slot < count)
        def _():
            raw_copy(slot).wait()

    def normalize(slot, piece):
        source = raw[slot, pl.ds(piece * PIECE, PIECE), :]
        widened = source.astype(jnp.float32)
        square_mean = jnp.mean(widened * widened, axis=-1, keepdims=True)
        scaled = widened * lax.rsqrt(square_mean + 1e-05) * half_gain[...]
        normed[slot, pl.ds(piece * PIECE, PIECE), :] = scaled.astype(jnp.bfloat16)

    def normalize_block(slot):
        for piece in range(BLOCK // PIECE):
            normalize(slot, piece)

    def scored(group, chunk, total):
        rows = normed[pl.ds(2 * group, 2)].reshape(2 * BLOCK, features)
        hidden = jnp.dot(
            rows,
            held[:, pl.ds(pl.multiple_of(chunk * CHUNK, CHUNK), CHUNK)],
            preferred_element_type=jnp.float32,
        )
        for k in range(CHUNK // BLOCK):
            here = hidden[:, k * BLOCK : (k + 1) * BLOCK]
            active = (here + here * jnp.tanh(here)).astype(jnp.bfloat16)
            line = pl.ds(chunk * (CHUNK // BLOCK) + k, 1)
            total += active.astype(jnp.float32) * head_rows[line, :]
        return total

    def finish(group):
        for side in range(2):
            slot = 2 * group + side
            scores = jnp.sum(sums[slot].T, axis=0, keepdims=True)
            target = jnp.where(slot < count, listed[0, 0, slot], spare)
            fresh[pl.ds(target, 1), :] = scores

    def first_groups(c, carry):
        held_copy(c).wait()
        wait_raw(2 * lead + c)
        for group in range(lead):
            both = pl.ds(2 * group, 2)
            before = sums[both].reshape(2 * BLOCK, BLOCK)
            sums[both] = scored(group, c, before).reshape(2, BLOCK, BLOCK)
        normalize_block(2 * lead + c)
        return carry

    def later_group(group, carry):
        total = jnp.zeros((2 * BLOCK, BLOCK), jnp.float32)
        finish(group - lead)
        for c in range(chunks):
            total = scored(group, c, total)
        sums[pl.ds(2 * group, 2)] = total.reshape(2, BLOCK, BLOCK)
        return carry

    @pl.when(count > 0)
    def _():
        for slot in range(2 * lead):
            start_raw(slot)
        for c in range(chunks):
            held_copy(c).start()
            start_raw(2 * lead + c)

    for e in range(env_rows):
        for k in range(per_row):
            row, part = pl.ds(e * per_row + k, 1), pl.ds(k * BLOCK, BLOCK)
            fresh[row, :] = stored[e : e + 1, part]
            packed[0, row, :] = rewards[e : e + 1, part]
            packed[1, row, :] = 1.0 - ends[e : e + 1, part].astype(jnp.float32)

    @pl.when(count > 0)
    def _():
        half_gain[...] = 0.5 * gain[...]
        head_rows[...] = head[...].astype(jnp.float32)
        sums[pl.ds(0, 2 * lead)] = jnp.zeros((2 * lead, BLOCK, BLOCK), jnp.float32)
        for slot in range(2 * lead):
            wait_raw(slot)
            normalize_block(slot)
        lax.fori_loop(0, chunks, first_groups, 0)
        lax.fori_loop(lead, groups, later_group, 0)
        finish(jnp.maximum(groups - lead, 0))
        finish(groups - 1)

    rows = fresh.shape[0]
    half = per_row
    value = fresh[...]
    lane = lax.broadcasted_iota(jnp.int32, (rows, BLOCK), 1)
    row = lax.broadcasted_iota(jnp.int32, (rows, BLOCK), 0)
    place = jnp.where(row < half, row, row - half)
    discount = 1.0 - 1.0 / spread((discount_horizon[0], discount_horizon[1]), rows, half)
    trace = 1.0 - 1.0 / spread((trace_horizon[0], trace_horizon[1]), rows, half)
    live = row < env_rows * half
    reward = jnp.where(live, packed[0], 0.0)
    going = jnp.where(live, packed[1], 0.0)
    value = jnp.where(live, value, 0.0)
    turned = shifted_left(value, 1)
    following = jnp.where(lane < BLOCK - 1, turned, shifted_up(turned, 1))
    last = (lane == BLOCK - 1) & (place == half - 1)
    following = jnp.where(last, value, following)
    factor = discount * trace * going
    offset = reward + discount * going * following - value
    by = 1
    while by < BLOCK:
        inside = lane < BLOCK - by
        offset = offset + factor * jnp.where(inside, shifted_left(offset, by), 0.0)
        factor = factor * jnp.where(inside, shifted_left(factor, by), 1.0)
        by *= 2
    row_factor = jnp.broadcast_to(factor[:, :1], (rows, BLOCK))
    row_offset = jnp.broadcast_to(offset[:, :1], (rows, BLOCK))
    by = 1
    while by < half:
        inside = place + by < half
        row_offset = row_offset + row_factor * jnp.where(
            inside, shifted_up(row_offset, by), 0.0
        )
        row_factor = row_factor * jnp.where(inside, shifted_up(row_factor, by), 1.0)
        by *= 2
    inside = place + 1 < half
    offset = offset + factor * jnp.where(inside, shifted_up(row_offset, 1), 0.0)
    factor = factor * jnp.where(inside, shifted_up(row_factor, 1), 1.0)

    packed[0] = offset
    packed[1] = factor
    fresh[...] = value
    lanes = lax.broadcasted_iota(jnp.int32, (1, BLOCK), 1)
    line = jnp.zeros((1, BLOCK), jnp.float32)
    for e in range(env_rows):
        mine = live & (row >= e * half) & (row < (e + 1) * half)

        def mean_of(array):
            return jnp.sum(jnp.where(mine, array, 0.0), keepdims=True) / steps

        mean_offset, mean_factor = mean_of(offset), mean_of(factor)
        near, far = offset - mean_offset, factor - mean_factor
        items = (
            row_offset[e * half : e * half + 1, :1],
            row_factor[e * half : e * half + 1, :1],
            value[e * half : e * half + 1, :1],
            value[(e + 1) * half - 1 : (e + 1) * half, BLOCK - 1 :],
            mean_offset,
            mean_factor,
            mean_of(near * near),
            mean_of(near * far),
            mean_of(far * far),
            1.0 / trace[e * half : e * half + 1, :1],
            jnp.full((1, 1), bootstrap[e], jnp.float32),
        )
        for k, item in enumerate(items):
            line = jnp.where(lanes == e * FIELDS + k, item, line)
        for k in range(per_row):
            source, part = pl.ds(e * per_row + k, 1), pl.ds(k * BLOCK, BLOCK)
            offset_ref[e : e + 1, part] = packed[0, source, :]
            factor_ref[e : e + 1, part] = packed[1, source, :]
            value_ref[e : e + 1, part] = fresh[source, :]
    message_ref[...] = line.reshape(message_ref.shape)


def exchange_kernel(
    shards,
    message,
    offset_ref,
    factor_ref,
    value_ref,
    result,
    gathered,
    partial,
    joined,
    send_sem,
    recv_sem,
    partial_sem,
    joined_sem,
):
    env, tm = lax.axis_index("env"), lax.axis_index("tm")
    envs = joined.shape[0]
    barrier = pltpu.get_barrier_semaphore()

    def each_shard(act):
        def one(i, carry):
            act(env, (tm + shards // 2 + i) % shards)
            return carry

        lax.fori_loop(0, shards // 2, one, 0)
        lax.fori_loop(shards // 2 + 1, shards, one, 0)

    def each_env(act):
        def one(i, carry):
            act((env + envs // 2 + i) % envs, tm)
            return carry

        lax.fori_loop(0, envs // 2, one, 0)
        lax.fori_loop(envs // 2 + 1, envs, one, 0)

    def greet(to_env, to_tm):
        pl.semaphore_signal(
            barrier, inc=1, device_id=(to_env, to_tm), device_id_type=MESH
        )

    def send(source, target, own, start_sem, end_sem):
        def act(to_env, to_tm):
            pltpu.make_async_remote_copy(
                src_ref=source,
                dst_ref=target.at[pl.ds(own, 1)],
                send_sem=start_sem,
                recv_sem=end_sem,
                device_id=(to_env, to_tm),
                device_id_type=MESH,
            ).start()

        return act

    def settle(target, length, sem):
        part = target.at[pl.ds(0, length)]
        pltpu.make_async_copy(part, part, sem).wait()

    each_shard(greet)
    each_env(greet)
    pl.semaphore_wait(barrier, shards + envs - 2)
    each_shard(send(message, gathered, tm, send_sem, recv_sem))
    gathered[pl.ds(tm, 1)] = message[...]
    settle(gathered, shards - 1, recv_sem)

    fields = gathered[...].reshape(shards, BLOCK)
    shard = lax.broadcasted_iota(jnp.int32, (shards, BLOCK), 0)
    lane = lax.broadcasted_iota(jnp.int32, (shards, BLOCK), 1)

    def field(k):
        return shifted_left(fields, k) if k else fields

    offset, factor, last = field(0), field(1), field(3)
    following = jnp.where(shard < shards - 1, shifted_up(field(2), 1), field(10))
    jump = (following - last) * field(9)
    reached = offset + factor * jump
    by = 1
    while by < shards:
        inside = shard + by < shards
        reached = reached + factor * jnp.where(inside, shifted_up(reached, by), 0.0)
        factor = factor * jnp.where(inside, shifted_up(factor, by), 1.0)
        by *= 2
    entering = jump + jnp.where(shard < shards - 1, shifted_up(reached, 1), 0.0)
    mean = field(4) + entering * field(5)
    inner = field(6) + entering * (2.0 * field(7) + entering * field(8))
    counted = (lane == 0) | (lane == FIELDS)

    def over_rows(array):
        return jnp.sum(jnp.where(counted, array, 0.0), keepdims=True) / (2 * shards)

    env_mean = over_rows(mean)
    off = mean - env_mean
    env_var = over_rows(inner + off * off)
    place = lax.broadcasted_iota(jnp.int32, (1, BLOCK), 1)
    line = jnp.where(place == 0, env_mean, jnp.where(place == 1, env_var, 0.0))
    partial[...] = line.reshape(partial.shape)
    own = jnp.sum(jnp.where(shard == tm, entering, 0.0), axis=0, keepdims=True)
    pair = lax.broadcasted_iota(jnp.int32, offset_ref.shape, 0)
    own = jnp.where(pair == 0, own[:, :1], own[:, FIELDS : FIELDS + 1])
    advantage = offset_ref[...] + factor_ref[...] * own
    result[0] = advantage + value_ref[...]
    each_env(send(partial, joined, env, partial_sem, joined_sem))
    joined[pl.ds(env, 1)] = partial[...]
    settle(joined, envs - 1, joined_sem)

    both = joined[...].reshape(envs, BLOCK)
    means, spans = both[:, :1], both[:, 1:2]
    adv_mean = jnp.sum(means, keepdims=True) / envs
    away = means - adv_mean
    adv_var = jnp.sum(spans + away * away, keepdims=True) / envs
    result[1] = (advantage - adv_mean) * lax.rsqrt(adv_var + 1e-05)
    settle(gathered, shards - 1, send_sem)
    settle(joined, envs - 1, partial_sem)


def on_device(
    observations,
    stored_values,
    rewards,
    episode_ends,
    stale_list,
    discount_horizon,
    trace_horizon,
    bootstrap,
    norm_gain,
    input_weight,
    value_head,
):
    env_rows, steps, features = observations.shape
    slots = env_rows * steps // BLOCK
    width = input_weight.shape[1]
    shape = pltpu.VMEM((env_rows, steps), jnp.float32)
    in_space = pltpu.with_memory_space_constraint
    vmem, smem, anywhere = (
        pl.BlockSpec(memory_space=pltpu.VMEM),
        pl.BlockSpec(memory_space=pltpu.SMEM),
        pl.BlockSpec(memory_space=pltpu.HBM),
    )
    offset, factor, value, message = pl.pallas_call(
        sweep_kernel,
        name="sweep",
        out_shape=(shape, shape, shape, pltpu.VMEM((1, 1, BLOCK), jnp.float32)),
        in_specs=[smem] * 4 + [anywhere] * 2 + [vmem] * 5,
        out_specs=[vmem] * 4,
        scratch_shapes=[
            pltpu.VMEM((slots, BLOCK, features), jnp.bfloat16),
            pltpu.VMEM((features, width), jnp.bfloat16),
            pltpu.VMEM((slots, BLOCK, features), jnp.bfloat16),
            pltpu.VMEM((slots, BLOCK, BLOCK), jnp.float32),
            pltpu.VMEM((16, BLOCK), jnp.float32),
            pltpu.VMEM((2, 16, BLOCK), jnp.float32),
            pltpu.VMEM((1, features), jnp.float32),
            pltpu.VMEM((width // BLOCK, BLOCK), jnp.float32),
            pltpu.SemaphoreType.DMA((slots,)),
            pltpu.SemaphoreType.DMA((width // CHUNK,)),
        ],
        compiler_params=pltpu.CompilerParams(vmem_limit_bytes=57 * 1024 * 1024),
    )(
        stale_list,
        discount_horizon,
        trace_horizon,
        bootstrap,
        in_space(observations.reshape(slots, BLOCK, features), pltpu.HBM),
        in_space(input_weight, pltpu.HBM),
        stored_values,
        rewards,
        episode_ends,
        norm_gain.reshape(1, features),
        value_head.reshape(width // BLOCK, BLOCK),
    )
    envs, shards = lax.axis_size("env"), lax.axis_size("tm")
    joined = pl.pallas_call(
        functools.partial(exchange_kernel, shards),
        name="exchange",
        out_shape=pltpu.VMEM((2, env_rows, steps), jnp.float32),
        in_specs=[vmem] * 4,
        out_specs=vmem,
        scratch_shapes=[
            pltpu.VMEM((shards, 1, BLOCK), jnp.float32),
            pltpu.VMEM((1, 1, BLOCK), jnp.float32),
            pltpu.VMEM((envs, 1, BLOCK), jnp.float32),
        ]
        + [pltpu.SemaphoreType.DMA] * 4,
        compiler_params=pltpu.CompilerParams(
            collective_id=0, has_side_effects=True, vmem_limit_bytes=57 * 1024 * 1024
        ),
    )(*(in_space(array, pltpu.VMEM) for array in (message, offset, factor, value)))
    return joined[0], joined[1]


def solution(mesh):
    placed = (
        P("env", "tm", None),
        P("env", "tm"),
        P("env", "tm"),
        P("env", "tm"),
        P("env", "tm", None),
        P("env"),
        P("env"),
        P("env"),
        P(),
        P(),
        P(),
    )
    return jax.shard_map(
        on_device,
        mesh=mesh,
        in_specs=placed,
        out_specs=(P("env", "tm"), P("env", "tm")),
        check_vma=False,
    )
```

```python
import functools

import jax
import jax.numpy as jnp
from jax import lax
from jax.experimental import pallas as pl
from jax.experimental.pallas import tpu as pltpu
from jax.sharding import PartitionSpec as P

BLOCK = 128
CHUNK = 512
PIECE = 32
FIELDS = 16
MESH = pl.DeviceIdType.MESH


def spread(pair, rows, half):
    row = lax.broadcasted_iota(jnp.int32, (rows, BLOCK), 0)
    return jnp.where(row < half, pair[0], pair[1])


def shifted_left(value, by):
    return pltpu.roll(value, value.shape[1] - by, 1)


def shifted_up(value, by):
    return pltpu.roll(value, value.shape[0] - by, 0)


def sweep_kernel(
    listed,
    discount_horizon,
    trace_horizon,
    bootstrap,
    obs,
    weight,
    stored,
    rewards,
    ends,
    gain,
    head,
    offset_ref,
    factor_ref,
    value_ref,
    message_ref,
    raw,
    held,
    normed,
    sums,
    fresh,
    packed,
    half_gain,
    head_rows,
    raw_sem,
    held_sem,
):
    slots, _, features = raw.shape
    width = held.shape[1]
    chunks = width // CHUNK
    env_rows, steps = stored.shape
    per_row = steps // BLOCK
    count = jnp.int32(0)
    for j in range(slots):
        count += (listed[0, 0, j] >= 0).astype(jnp.int32)
    groups = (count + 1) // 2
    spare = fresh.shape[0] - 1

    def raw_copy(slot):
        block = jnp.maximum(listed[0, 0, slot], 0)
        return pltpu.make_async_copy(obs.at[block], raw.at[slot], raw_sem.at[slot])

    def held_copy(c):
        part = pl.ds(c * CHUNK, CHUNK)
        return pltpu.make_async_copy(
            weight.at[:, part], held.at[:, part], held_sem.at[c]
        )

    def start_raw(slot):
        @pl.when(slot < count)
        def _():
            raw_copy(slot).start()

    def wait_raw(slot):
        @pl.when(slot < count)
        def _():
            raw_copy(slot).wait()

    def normalize(slot, piece):
        source = raw[slot, pl.ds(piece * PIECE, PIECE), :]
        widened = source.astype(jnp.float32)
        square_mean = jnp.mean(widened * widened, axis=-1, keepdims=True)
        scaled = widened * lax.rsqrt(square_mean + 1e-05) * half_gain[...]
        normed[slot, pl.ds(piece * PIECE, PIECE), :] = scaled.astype(jnp.bfloat16)

    def normalize_block(slot):
        for piece in range(BLOCK // PIECE):
            normalize(slot, piece)

    def scored(group, chunk, total):
        rows = normed[pl.ds(2 * group, 2)].reshape(2 * BLOCK, features)
        hidden = jnp.dot(
            rows,
            held[:, pl.ds(pl.multiple_of(chunk * CHUNK, CHUNK), CHUNK)],
            preferred_element_type=jnp.float32,
        )
        for k in range(CHUNK // BLOCK):
            here = hidden[:, k * BLOCK : (k + 1) * BLOCK]
            active = (here + here * jnp.tanh(here)).astype(jnp.bfloat16)
            line = pl.ds(chunk * (CHUNK // BLOCK) + k, 1)
            total += active.astype(jnp.float32) * head_rows[line, :]
        return total

    def finish(group):
        for side in range(2):
            slot = 2 * group + side
            scores = jnp.sum(sums[slot].T, axis=0, keepdims=True)
            target = jnp.where(slot < count, listed[0, 0, slot], spare)
            fresh[pl.ds(target, 1), :] = scores

    def add_chunk(group, c):
        both = pl.ds(2 * group, 2)
        before = sums[both].reshape(2 * BLOCK, BLOCK)
        sums[both] = scored(group, c, before).reshape(2, BLOCK, BLOCK)

    def first_groups(c, carry):
        held_copy(c + 1).wait()
        wait_raw(4 + c)
        add_chunk(1, c)
        add_chunk(0, c + 1)
        normalize_block(4 + c)
        return carry

    def later_group(group, carry):
        total = jnp.zeros((2 * BLOCK, BLOCK), jnp.float32)
        finish(group - 2)
        finish(group - 1)
        for c in range(chunks):
            total = scored(group, c, total)
        sums[pl.ds(2 * group, 2)] = total.reshape(2, BLOCK, BLOCK)
        return carry

    @pl.when(count > 0)
    def _():
        for slot in range(2):
            start_raw(slot)
        held_copy(0).start()
        for slot in range(2, 4):
            start_raw(slot)
        for c in range(1, chunks):
            held_copy(c).start()
            start_raw(3 + c)
        start_raw(slots - 1)

    for e in range(env_rows):
        for k in range(per_row):
            row, part = pl.ds(e * per_row + k, 1), pl.ds(k * BLOCK, BLOCK)
            fresh[row, :] = stored[e : e + 1, part]
            packed[0, row, :] = rewards[e : e + 1, part]
            packed[1, row, :] = 1.0 - ends[e : e + 1, part].astype(jnp.float32)

    @pl.when(count > 0)
    def _():
        half_gain[...] = 0.5 * gain[...]
        head_rows[...] = head[...].astype(jnp.float32)
        sums[pl.ds(0, 4)] = jnp.zeros((4, BLOCK, BLOCK), jnp.float32)
        for slot in range(2):
            wait_raw(slot)
            normalize_block(slot)
        held_copy(0).wait()
        for slot in range(2, 4):
            wait_raw(slot)
        add_chunk(0, 0)
        for slot in range(2, 4):
            normalize_block(slot)
        lax.fori_loop(0, chunks - 1, first_groups, 0)
        wait_raw(slots - 1)
        add_chunk(1, chunks - 1)
        normalize_block(slots - 1)
        lax.fori_loop(2, groups, later_group, 0)

        @pl.when(groups <= 2)
        def _():
            finish(0)

        finish(groups - 1)

    rows = fresh.shape[0]
    half = per_row
    value = fresh[...]
    lane = lax.broadcasted_iota(jnp.int32, (rows, BLOCK), 1)
    row = lax.broadcasted_iota(jnp.int32, (rows, BLOCK), 0)
    place = jnp.where(row < half, row, row - half)
    discount = 1.0 - 1.0 / spread((discount_horizon[0], discount_horizon[1]), rows, half)
    trace = 1.0 - 1.0 / spread((trace_horizon[0], trace_horizon[1]), rows, half)
    live = row < env_rows * half
    reward = jnp.where(live, packed[0], 0.0)
    going = jnp.where(live, packed[1], 0.0)
    value = jnp.where(live, value, 0.0)
    turned = shifted_left(value, 1)
    following = jnp.where(lane < BLOCK - 1, turned, shifted_up(turned, 1))
    last = (lane == BLOCK - 1) & (place == half - 1)
    following = jnp.where(last, value, following)
    factor = discount * trace * going
    offset = reward + discount * going * following - value
    by = 1
    while by < BLOCK:
        inside = lane < BLOCK - by
        offset = offset + factor * jnp.where(inside, shifted_left(offset, by), 0.0)
        factor = factor * jnp.where(inside, shifted_left(factor, by), 1.0)
        by *= 2
    row_factor = jnp.broadcast_to(factor[:, :1], (rows, BLOCK))
    row_offset = jnp.broadcast_to(offset[:, :1], (rows, BLOCK))
    by = 1
    while by < half:
        inside = place + by < half
        row_offset = row_offset + row_factor * jnp.where(
            inside, shifted_up(row_offset, by), 0.0
        )
        row_factor = row_factor * jnp.where(inside, shifted_up(row_factor, by), 1.0)
        by *= 2
    inside = place + 1 < half
    offset = offset + factor * jnp.where(inside, shifted_up(row_offset, 1), 0.0)
    factor = factor * jnp.where(inside, shifted_up(row_factor, 1), 1.0)

    packed[0] = offset
    packed[1] = factor
    fresh[...] = value
    lanes = lax.broadcasted_iota(jnp.int32, (1, BLOCK), 1)
    line = jnp.zeros((1, BLOCK), jnp.float32)
    for e in range(env_rows):
        mine = live & (row >= e * half) & (row < (e + 1) * half)

        def mean_of(array):
            return jnp.sum(jnp.where(mine, array, 0.0), keepdims=True) / steps

        first_offset = row_offset[e * half : e * half + 1, :1]
        first_factor = row_factor[e * half : e * half + 1, :1]
        near, far = offset - first_offset, factor - first_factor
        mean_near, mean_far = mean_of(near), mean_of(far)
        items = (
            first_offset,
            first_factor,
            value[e * half : e * half + 1, :1],
            value[(e + 1) * half - 1 : (e + 1) * half, BLOCK - 1 :],
            first_offset + mean_near,
            first_factor + mean_far,
            mean_of(near * near) - mean_near * mean_near,
            mean_of(near * far) - mean_near * mean_far,
            mean_of(far * far) - mean_far * mean_far,
            1.0 / trace[e * half : e * half + 1, :1],
            jnp.full((1, 1), bootstrap[e], jnp.float32),
        )
        for k, item in enumerate(items):
            line = jnp.where(lanes == e * FIELDS + k, item, line)
        for k in range(per_row):
            source, part = pl.ds(e * per_row + k, 1), pl.ds(k * BLOCK, BLOCK)
            offset_ref[e : e + 1, part] = packed[0, source, :]
            factor_ref[e : e + 1, part] = packed[1, source, :]
            value_ref[e : e + 1, part] = fresh[source, :]
    message_ref[...] = line.reshape(message_ref.shape)


def exchange_kernel(
    shards,
    message,
    offset_ref,
    factor_ref,
    value_ref,
    result,
    gathered,
    partial,
    joined,
    send_sem,
    recv_sem,
    partial_sem,
    joined_sem,
):
    env, tm = lax.axis_index("env"), lax.axis_index("tm")
    envs = joined.shape[0]
    barrier = pltpu.get_barrier_semaphore()

    def each_shard(act):
        for i in range(1, shards):
            act(env, (tm + i * (shards // 2 + 1)) % shards)

    def each_env(act):
        for i in range(1, envs):
            act((env + i * (envs // 2 + 1)) % envs, tm)

    def greet(to_env, to_tm):
        pl.semaphore_signal(
            barrier, inc=1, device_id=(to_env, to_tm), device_id_type=MESH
        )

    def send(source, target, own, start_sem, end_sem):
        def act(to_env, to_tm):
            pltpu.make_async_remote_copy(
                src_ref=source,
                dst_ref=target.at[pl.ds(own, 1)],
                send_sem=start_sem,
                recv_sem=end_sem,
                device_id=(to_env, to_tm),
                device_id_type=MESH,
            ).start()

        return act

    def settle(target, length, sem):
        part = target.at[pl.ds(0, length)]
        pltpu.make_async_copy(part, part, sem).wait()

    each_shard(greet)
    each_env(greet)
    pl.semaphore_wait(barrier, shards + envs - 2)
    each_shard(send(message, gathered, tm, send_sem, recv_sem))
    gathered[pl.ds(tm, 1)] = message[...]
    settle(gathered, shards - 1, recv_sem)

    fields = gathered[...].reshape(shards, BLOCK)
    shard = lax.broadcasted_iota(jnp.int32, (shards, BLOCK), 0)
    lane = lax.broadcasted_iota(jnp.int32, (shards, BLOCK), 1)

    def field(k):
        return shifted_left(fields, k) if k else fields

    offset, factor, last = field(0), field(1), field(3)
    following = jnp.where(shard < shards - 1, shifted_up(field(2), 1), field(10))
    jump = (following - last) * field(9)
    reached = offset + factor * jump
    by = 1
    while by < shards:
        inside = shard + by < shards
        reached = reached + factor * jnp.where(inside, shifted_up(reached, by), 0.0)
        factor = factor * jnp.where(inside, shifted_up(factor, by), 1.0)
        by *= 2
    entering = jump + jnp.where(shard < shards - 1, shifted_up(reached, 1), 0.0)
    mean = field(4) + entering * field(5)
    inner = field(6) + entering * (2.0 * field(7) + entering * field(8))
    counted = (lane == 0) | (lane == FIELDS)

    def over_rows(array):
        return jnp.sum(jnp.where(counted, array, 0.0), keepdims=True) / (2 * shards)

    env_mean = over_rows(mean)
    off = mean - env_mean
    env_var = over_rows(inner + off * off)
    place = lax.broadcasted_iota(jnp.int32, (1, BLOCK), 1)
    line = jnp.where(place == 0, env_mean, jnp.where(place == 1, env_var, 0.0))
    partial[...] = line.reshape(partial.shape)
    own = jnp.sum(jnp.where(shard == tm, entering, 0.0), axis=0, keepdims=True)
    pair = lax.broadcasted_iota(jnp.int32, offset_ref.shape, 0)
    own = jnp.where(pair == 0, own[:, :1], own[:, FIELDS : FIELDS + 1])
    advantage = offset_ref[...] + factor_ref[...] * own
    result[0] = advantage + value_ref[...]
    each_env(send(partial, joined, env, partial_sem, joined_sem))
    joined[pl.ds(env, 1)] = partial[...]
    settle(joined, envs - 1, joined_sem)

    both = joined[...].reshape(envs, BLOCK)
    means, spans = both[:, :1], both[:, 1:2]
    adv_mean = jnp.sum(means, keepdims=True) / envs
    away = means - adv_mean
    adv_var = jnp.sum(spans + away * away, keepdims=True) / envs
    result[1] = (advantage - adv_mean) * lax.rsqrt(adv_var + 1e-05)
    settle(gathered, shards - 1, send_sem)
    settle(joined, envs - 1, partial_sem)


def on_device(
    observations,
    stored_values,
    rewards,
    episode_ends,
    stale_list,
    discount_horizon,
    trace_horizon,
    bootstrap,
    norm_gain,
    input_weight,
    value_head,
):
    env_rows, steps, features = observations.shape
    slots = env_rows * steps // BLOCK
    width = input_weight.shape[1]
    shape = pltpu.VMEM((env_rows, steps), jnp.float32)
    in_space = pltpu.with_memory_space_constraint
    vmem, smem, anywhere = (
        pl.BlockSpec(memory_space=pltpu.VMEM),
        pl.BlockSpec(memory_space=pltpu.SMEM),
        pl.BlockSpec(memory_space=pltpu.HBM),
    )
    offset, factor, value, message = pl.pallas_call(
        sweep_kernel,
        name="sweep",
        out_shape=(shape, shape, shape, pltpu.VMEM((1, 1, BLOCK), jnp.float32)),
        in_specs=[smem] * 4 + [anywhere] * 2 + [vmem] * 5,
        out_specs=[vmem] * 4,
        scratch_shapes=[
            pltpu.VMEM((slots, BLOCK, features), jnp.bfloat16),
            pltpu.VMEM((features, width), jnp.bfloat16),
            pltpu.VMEM((slots, BLOCK, features), jnp.bfloat16),
            pltpu.VMEM((slots, BLOCK, BLOCK), jnp.float32),
            pltpu.VMEM((16, BLOCK), jnp.float32),
            pltpu.VMEM((2, 16, BLOCK), jnp.float32),
            pltpu.VMEM((1, features), jnp.float32),
            pltpu.VMEM((width // BLOCK, BLOCK), jnp.float32),
            pltpu.SemaphoreType.DMA((slots,)),
            pltpu.SemaphoreType.DMA((width // CHUNK,)),
        ],
        compiler_params=pltpu.CompilerParams(vmem_limit_bytes=57 * 1024 * 1024),
    )(
        stale_list,
        discount_horizon,
        trace_horizon,
        bootstrap,
        in_space(observations.reshape(slots, BLOCK, features), pltpu.HBM),
        in_space(input_weight, pltpu.HBM),
        stored_values,
        rewards,
        episode_ends,
        norm_gain.reshape(1, features),
        value_head.reshape(width // BLOCK, BLOCK),
    )
    envs, shards = lax.axis_size("env"), lax.axis_size("tm")
    joined = pl.pallas_call(
        functools.partial(exchange_kernel, shards),
        name="exchange",
        out_shape=pltpu.VMEM((2, env_rows, steps), jnp.float32),
        in_specs=[vmem] * 4,
        out_specs=vmem,
        scratch_shapes=[
            pltpu.VMEM((shards, 1, BLOCK), jnp.float32),
            pltpu.VMEM((1, 1, BLOCK), jnp.float32),
            pltpu.VMEM((envs, 1, BLOCK), jnp.float32),
        ]
        + [pltpu.SemaphoreType.DMA] * 4,
        compiler_params=pltpu.CompilerParams(
            collective_id=0, has_side_effects=True, vmem_limit_bytes=57 * 1024 * 1024
        ),
    )(*(in_space(array, pltpu.VMEM) for array in (message, offset, factor, value)))
    return joined[0], joined[1]


def solution(mesh):
    placed = (
        P("env", "tm", None),
        P("env", "tm"),
        P("env", "tm"),
        P("env", "tm"),
        P("env", "tm", None),
        P("env"),
        P("env"),
        P("env"),
        P(),
        P(),
        P(),
    )
    return jax.shard_map(
        on_device,
        mesh=mesh,
        in_specs=placed,
        out_specs=(P("env", "tm"), P("env", "tm")),
        check_vma=False,
    )
```

```python
import functools

import jax
import jax.numpy as jnp
from jax import lax
from jax.experimental import pallas as pl
from jax.experimental.pallas import tpu as pltpu
from jax.sharding import PartitionSpec as P

BLOCK = 128
CHUNK = 512
PIECE = 32
FIELDS = 16
MESH = pl.DeviceIdType.MESH


def spread(pair, rows, half):
    row = lax.broadcasted_iota(jnp.int32, (rows, BLOCK), 0)
    return jnp.where(row < half, pair[0], pair[1])


def shifted_left(value, by):
    return pltpu.roll(value, value.shape[1] - by, 1)


def shifted_up(value, by):
    return pltpu.roll(value, value.shape[0] - by, 0)


def sweep_kernel(
    listed,
    discount_horizon,
    trace_horizon,
    bootstrap,
    obs,
    weight,
    stored_in,
    rewards_in,
    ends_in,
    gain_in,
    head_in,
    offset_ref,
    factor_ref,
    value_ref,
    message_ref,
    raw,
    held,
    normed,
    sums,
    fresh,
    packed,
    half_gain,
    head_rows,
    stored,
    rewards,
    ends,
    gain,
    head,
    raw_sem,
    held_sem,
    small_sem,
):
    loads = [
        pltpu.make_async_copy(source, target, small_sem.at[k])
        for k, (source, target) in enumerate(
            (
                (stored_in, stored),
                (rewards_in, rewards),
                (ends_in, ends),
                (gain_in, gain),
                (head_in, head),
            )
        )
    ]
    for load in loads:
        load.start()
    slots, _, features = raw.shape
    width = held.shape[1]
    chunks = width // CHUNK
    env_rows, steps = stored.shape
    per_row = steps // BLOCK
    count = jnp.int32(0)
    for j in range(slots):
        count += (listed[0, 0, j] >= 0).astype(jnp.int32)
    groups = (count + 1) // 2
    spare = fresh.shape[0] - 1

    def raw_copy(slot):
        block = jnp.maximum(listed[0, 0, slot], 0)
        return pltpu.make_async_copy(obs.at[block], raw.at[slot], raw_sem.at[slot])

    def held_copy(c):
        part = pl.ds(c * CHUNK, CHUNK)
        return pltpu.make_async_copy(
            weight.at[:, part], held.at[:, part], held_sem.at[c]
        )

    def start_raw(slot):
        @pl.when(slot < count)
        def _():
            raw_copy(slot).start()

    def wait_raw(slot):
        @pl.when(slot < count)
        def _():
            raw_copy(slot).wait()

    def normalize(slot, piece):
        source = raw[slot, pl.ds(piece * PIECE, PIECE), :]
        widened = source.astype(jnp.float32)
        square_mean = jnp.mean(widened * widened, axis=-1, keepdims=True)
        scaled = widened * lax.rsqrt(square_mean + 1e-05) * half_gain[...]
        normed[slot, pl.ds(piece * PIECE, PIECE), :] = scaled.astype(jnp.bfloat16)

    def normalize_block(slot):
        for piece in range(BLOCK // PIECE):
            normalize(slot, piece)

    def scored(group, chunk, total):
        rows = normed[pl.ds(2 * group, 2)].reshape(2 * BLOCK, features)
        hidden = jnp.dot(
            rows,
            held[:, pl.ds(pl.multiple_of(chunk * CHUNK, CHUNK), CHUNK)],
            preferred_element_type=jnp.float32,
        )
        for k in range(CHUNK // BLOCK):
            here = hidden[:, k * BLOCK : (k + 1) * BLOCK]
            active = (here + here * jnp.tanh(here)).astype(jnp.bfloat16)
            line = pl.ds(chunk * (CHUNK // BLOCK) + k, 1)
            total += active.astype(jnp.float32) * head_rows[line, :]
        return total

    def finish(group):
        for side in range(2):
            slot = 2 * group + side
            scores = jnp.sum(sums[slot].T, axis=0, keepdims=True)
            target = jnp.where(slot < count, listed[0, 0, slot], spare)
            fresh[pl.ds(target, 1), :] = scores

    def add_chunk(group, c):
        both = pl.ds(2 * group, 2)
        before = sums[both].reshape(2 * BLOCK, BLOCK)
        sums[both] = scored(group, c, before).reshape(2, BLOCK, BLOCK)

    def first_groups(c, carry):
        held_copy(c + 1).wait()
        wait_raw(4 + c)
        add_chunk(1, c)
        add_chunk(0, c + 1)
        normalize_block(4 + c)
        return carry

    def later_group(group, carry):
        total = jnp.zeros((2 * BLOCK, BLOCK), jnp.float32)
        finish(group - 2)
        finish(group - 1)
        for c in range(chunks):
            total = scored(group, c, total)
        sums[pl.ds(2 * group, 2)] = total.reshape(2, BLOCK, BLOCK)
        return carry

    @pl.when(count > 0)
    def _():
        for slot in range(2):
            start_raw(slot)
        held_copy(0).start()
        for slot in range(2, 4):
            start_raw(slot)
        for c in range(1, chunks):
            held_copy(c).start()
            start_raw(3 + c)
        start_raw(slots - 1)

    for load in loads:
        load.wait()
    for e in range(env_rows):
        for k in range(per_row):
            row, part = pl.ds(e * per_row + k, 1), pl.ds(k * BLOCK, BLOCK)
            fresh[row, :] = stored[e : e + 1, part]
            packed[0, row, :] = rewards[e : e + 1, part]
            packed[1, row, :] = 1.0 - ends[e : e + 1, part].astype(jnp.float32)

    @pl.when(count > 0)
    def _():
        half_gain[...] = 0.5 * gain[...]
        head_rows[...] = head[...].astype(jnp.float32)
        sums[pl.ds(0, 4)] = jnp.zeros((4, BLOCK, BLOCK), jnp.float32)
        for slot in range(2):
            wait_raw(slot)
            normalize_block(slot)
        held_copy(0).wait()
        for slot in range(2, 4):
            wait_raw(slot)
        add_chunk(0, 0)
        for slot in range(2, 4):
            normalize_block(slot)
        lax.fori_loop(0, chunks - 1, first_groups, 0)
        wait_raw(slots - 1)
        add_chunk(1, chunks - 1)
        normalize_block(slots - 1)
        lax.fori_loop(2, groups, later_group, 0)

        @pl.when(groups <= 2)
        def _():
            finish(0)

        finish(groups - 1)

    rows = fresh.shape[0]
    half = per_row
    value = fresh[...]
    lane = lax.broadcasted_iota(jnp.int32, (rows, BLOCK), 1)
    row = lax.broadcasted_iota(jnp.int32, (rows, BLOCK), 0)
    place = jnp.where(row < half, row, row - half)
    discount = 1.0 - 1.0 / spread((discount_horizon[0], discount_horizon[1]), rows, half)
    trace = 1.0 - 1.0 / spread((trace_horizon[0], trace_horizon[1]), rows, half)
    live = row < env_rows * half
    reward = jnp.where(live, packed[0], 0.0)
    going = jnp.where(live, packed[1], 0.0)
    value = jnp.where(live, value, 0.0)
    turned = shifted_left(value, 1)
    following = jnp.where(lane < BLOCK - 1, turned, shifted_up(turned, 1))
    last = (lane == BLOCK - 1) & (place == half - 1)
    following = jnp.where(last, value, following)
    factor = discount * trace * going
    offset = reward + discount * going * following - value
    by = 1
    while by < BLOCK:
        inside = lane < BLOCK - by
        offset = offset + factor * jnp.where(inside, shifted_left(offset, by), 0.0)
        factor = factor * jnp.where(inside, shifted_left(factor, by), 1.0)
        by *= 2
    row_factor = jnp.broadcast_to(factor[:, :1], (rows, BLOCK))
    row_offset = jnp.broadcast_to(offset[:, :1], (rows, BLOCK))
    by = 1
    while by < half:
        inside = place + by < half
        row_offset = row_offset + row_factor * jnp.where(
            inside, shifted_up(row_offset, by), 0.0
        )
        row_factor = row_factor * jnp.where(inside, shifted_up(row_factor, by), 1.0)
        by *= 2
    inside = place + 1 < half
    offset = offset + factor * jnp.where(inside, shifted_up(row_offset, 1), 0.0)
    factor = factor * jnp.where(inside, shifted_up(row_factor, 1), 1.0)

    packed[0] = offset
    packed[1] = factor
    fresh[...] = value
    lanes = lax.broadcasted_iota(jnp.int32, (1, BLOCK), 1)
    line = jnp.zeros((1, BLOCK), jnp.float32)
    for e in range(env_rows):
        mine = live & (row >= e * half) & (row < (e + 1) * half)

        def mean_of(array):
            return jnp.sum(jnp.where(mine, array, 0.0), keepdims=True) / steps

        first_offset = row_offset[e * half : e * half + 1, :1]
        first_factor = row_factor[e * half : e * half + 1, :1]
        near, far = offset - first_offset, factor - first_factor
        mean_near, mean_far = mean_of(near), mean_of(far)
        items = (
            first_offset,
            first_factor,
            value[e * half : e * half + 1, :1],
            value[(e + 1) * half - 1 : (e + 1) * half, BLOCK - 1 :],
            first_offset + mean_near,
            first_factor + mean_far,
            mean_of(near * near) - mean_near * mean_near,
            mean_of(near * far) - mean_near * mean_far,
            mean_of(far * far) - mean_far * mean_far,
            1.0 / trace[e * half : e * half + 1, :1],
            jnp.full((1, 1), bootstrap[e], jnp.float32),
        )
        for k, item in enumerate(items):
            line = jnp.where(lanes == e * FIELDS + k, item, line)
        for k in range(per_row):
            source, part = pl.ds(e * per_row + k, 1), pl.ds(k * BLOCK, BLOCK)
            offset_ref[e : e + 1, part] = packed[0, source, :]
            factor_ref[e : e + 1, part] = packed[1, source, :]
            value_ref[e : e + 1, part] = fresh[source, :]
    message_ref[...] = line.reshape(message_ref.shape)


def exchange_kernel(
    shards,
    message,
    offset_ref,
    factor_ref,
    value_ref,
    result,
    gathered,
    partial,
    joined,
    send_sem,
    recv_sem,
    partial_sem,
    joined_sem,
):
    env, tm = lax.axis_index("env"), lax.axis_index("tm")
    envs = joined.shape[0]
    barrier = pltpu.get_barrier_semaphore()

    def each_shard(act):
        for i in range(1, shards):
            act(env, (tm + i * (shards // 2 + 1)) % shards)

    def each_env(act):
        for i in range(1, envs):
            act((env + i * (envs // 2 + 1)) % envs, tm)

    def greet(to_env, to_tm):
        pl.semaphore_signal(
            barrier, inc=1, device_id=(to_env, to_tm), device_id_type=MESH
        )

    def send(source, target, own, start_sem, end_sem):
        def act(to_env, to_tm):
            pltpu.make_async_remote_copy(
                src_ref=source,
                dst_ref=target.at[pl.ds(own, 1)],
                send_sem=start_sem,
                recv_sem=end_sem,
                device_id=(to_env, to_tm),
                device_id_type=MESH,
            ).start()

        return act

    def settle(target, length, sem):
        part = target.at[pl.ds(0, length)]
        pltpu.make_async_copy(part, part, sem).wait()

    each_shard(greet)
    each_env(greet)
    pl.semaphore_wait(barrier, shards + envs - 2)
    each_shard(send(message, gathered, tm, send_sem, recv_sem))
    gathered[pl.ds(tm, 1)] = message[...]
    settle(gathered, shards - 1, recv_sem)

    fields = gathered[...].reshape(shards, BLOCK)
    shard = lax.broadcasted_iota(jnp.int32, (shards, BLOCK), 0)
    lane = lax.broadcasted_iota(jnp.int32, (shards, BLOCK), 1)

    def field(k):
        return shifted_left(fields, k) if k else fields

    offset, factor, last = field(0), field(1), field(3)
    following = jnp.where(shard < shards - 1, shifted_up(field(2), 1), field(10))
    jump = (following - last) * field(9)
    reached = offset + factor * jump
    by = 1
    while by < shards:
        inside = shard + by < shards
        reached = reached + factor * jnp.where(inside, shifted_up(reached, by), 0.0)
        factor = factor * jnp.where(inside, shifted_up(factor, by), 1.0)
        by *= 2
    entering = jump + jnp.where(shard < shards - 1, shifted_up(reached, 1), 0.0)
    mean = field(4) + entering * field(5)
    inner = field(6) + entering * (2.0 * field(7) + entering * field(8))
    counted = (lane == 0) | (lane == FIELDS)

    def over_rows(array):
        return jnp.sum(jnp.where(counted, array, 0.0), keepdims=True) / (2 * shards)

    env_mean = over_rows(mean)
    off = mean - env_mean
    env_var = over_rows(inner + off * off)
    place = lax.broadcasted_iota(jnp.int32, (1, BLOCK), 1)
    line = jnp.where(place == 0, env_mean, jnp.where(place == 1, env_var, 0.0))
    partial[...] = line.reshape(partial.shape)
    own = jnp.sum(jnp.where(shard == tm, entering, 0.0), axis=0, keepdims=True)
    pair = lax.broadcasted_iota(jnp.int32, offset_ref.shape, 0)
    own = jnp.where(pair == 0, own[:, :1], own[:, FIELDS : FIELDS + 1])
    advantage = offset_ref[...] + factor_ref[...] * own
    result[0] = advantage + value_ref[...]
    each_env(send(partial, joined, env, partial_sem, joined_sem))
    joined[pl.ds(env, 1)] = partial[...]
    settle(joined, envs - 1, joined_sem)

    both = joined[...].reshape(envs, BLOCK)
    means, spans = both[:, :1], both[:, 1:2]
    adv_mean = jnp.sum(means, keepdims=True) / envs
    away = means - adv_mean
    adv_var = jnp.sum(spans + away * away, keepdims=True) / envs
    result[1] = (advantage - adv_mean) * lax.rsqrt(adv_var + 1e-05)
    settle(gathered, shards - 1, send_sem)
    settle(joined, envs - 1, partial_sem)


def on_device(
    observations,
    stored_values,
    rewards,
    episode_ends,
    stale_list,
    discount_horizon,
    trace_horizon,
    bootstrap,
    norm_gain,
    input_weight,
    value_head,
):
    env_rows, steps, features = observations.shape
    slots = env_rows * steps // BLOCK
    width = input_weight.shape[1]
    shape = pltpu.VMEM((env_rows, steps), jnp.float32)
    in_space = pltpu.with_memory_space_constraint
    vmem, smem, anywhere = (
        pl.BlockSpec(memory_space=pltpu.VMEM),
        pl.BlockSpec(memory_space=pltpu.SMEM),
        pl.BlockSpec(memory_space=pltpu.HBM),
    )
    offset, factor, value, message = pl.pallas_call(
        sweep_kernel,
        name="sweep",
        out_shape=(shape, shape, shape, pltpu.VMEM((1, 1, BLOCK), jnp.float32)),
        in_specs=[smem] * 4 + [anywhere] * 7,
        out_specs=[vmem] * 4,
        scratch_shapes=[
            pltpu.VMEM((slots, BLOCK, features), jnp.bfloat16),
            pltpu.VMEM((features, width), jnp.bfloat16),
            pltpu.VMEM((slots, BLOCK, features), jnp.bfloat16),
            pltpu.VMEM((slots, BLOCK, BLOCK), jnp.float32),
            pltpu.VMEM((16, BLOCK), jnp.float32),
            pltpu.VMEM((2, 16, BLOCK), jnp.float32),
            pltpu.VMEM((1, features), jnp.float32),
            pltpu.VMEM((width // BLOCK, BLOCK), jnp.float32),
            pltpu.VMEM((env_rows, steps), jnp.float32),
            pltpu.VMEM((env_rows, steps), jnp.float32),
            pltpu.VMEM((env_rows, steps), jnp.int32),
            pltpu.VMEM((1, features), jnp.float32),
            pltpu.VMEM((width // BLOCK, BLOCK), jnp.bfloat16),
            pltpu.SemaphoreType.DMA((slots,)),
            pltpu.SemaphoreType.DMA((width // CHUNK,)),
            pltpu.SemaphoreType.DMA((5,)),
        ],
        compiler_params=pltpu.CompilerParams(vmem_limit_bytes=57 * 1024 * 1024),
    )(
        stale_list,
        discount_horizon,
        trace_horizon,
        bootstrap,
        in_space(observations.reshape(slots, BLOCK, features), pltpu.HBM),
        in_space(input_weight, pltpu.HBM),
        stored_values,
        rewards,
        episode_ends,
        norm_gain.reshape(1, features),
        value_head.reshape(width // BLOCK, BLOCK),
    )
    envs, shards = lax.axis_size("env"), lax.axis_size("tm")
    joined = pl.pallas_call(
        functools.partial(exchange_kernel, shards),
        name="exchange",
        out_shape=pltpu.VMEM((2, env_rows, steps), jnp.float32),
        in_specs=[vmem] * 4,
        out_specs=vmem,
        scratch_shapes=[
            pltpu.VMEM((shards, 1, BLOCK), jnp.float32),
            pltpu.VMEM((1, 1, BLOCK), jnp.float32),
            pltpu.VMEM((envs, 1, BLOCK), jnp.float32),
        ]
        + [pltpu.SemaphoreType.DMA] * 4,
        compiler_params=pltpu.CompilerParams(
            collective_id=0, has_side_effects=True, vmem_limit_bytes=57 * 1024 * 1024
        ),
    )(*(in_space(array, pltpu.VMEM) for array in (message, offset, factor, value)))
    return joined[0], joined[1]


def solution(mesh):
    placed = (
        P("env", "tm", None),
        P("env", "tm"),
        P("env", "tm"),
        P("env", "tm"),
        P("env", "tm", None),
        P("env"),
        P("env"),
        P("env"),
        P(),
        P(),
        P(),
    )
    return jax.shard_map(
        on_device,
        mesh=mesh,
        in_specs=placed,
        out_specs=(P("env", "tm"), P("env", "tm")),
        check_vma=False,
    )
```
